512 devices in a mesh: heads: 8 (over y_lo, x), blk: 64 (over y_hi, z, core).
Axes of the slice: x: 4, y: 8 (y_hi: 4, y_lo: 2; y = y_hi * 2 + y_lo), z: 8, core: 2. Of those that a mesh axis runs over, the one named last changes fastest.
Arguments:
- queries: bfloat16 [4096, 64, 128], P('blk', 'heads'), may hold values from -8 to 8
- prefix_keys: bfloat16 [8, 131072, 128], P('heads', 'blk'), may hold values from -8 to 8
- cached_prefix_values: bfloat16 [8, 131072, 128], P('heads', 'blk'), may hold values from -6 to 6
- shard_len: int32 [64], replicated, may hold values from 512 to 2048
- reach: int32 [64], replicated, may hold values from 4096 to 8192
- w_out: bfloat16 [8192, 16384], P('heads', 'blk'), may hold values from -0.0625 to 0.0625
Outputs:
- projected: bfloat16 [4096, 16384], P('heads', 'blk')
The draws below stay inside these ranges and needn't reach their ends.
All inputs are finite; a program needn't handle non-finite values.
Results may differ from the reference program's by a relative error of at most 0.0056.
Values may be sent and summed in bfloat16 or wider, within the bound.
No kernel may reach another device: no remote copies, remote signals or barrier semaphores. Data moves between devices by JAX's collectives and lax.ppermute only.
A program may use at most 64 MiB of HBM per device.

```python
import jax
import jax.numpy as jnp
from jax import lax

D = 16384
QUERY_HEADS = 64
KEY_VALUE_HEADS = 8
HEAD_DIM = 128
QUERY_TOKENS = 64
KEYS_DEV = 2048
SPAN = 4
SHARDS = 64
TOKENS = 4096
PREFIX_SLOTS = 131072


def draw_queries(key, part):
    random_seed_key = jax.random.fold_in(key, 1)
    random_sample = jnp.clip(jax.random.normal(random_seed_key, (TOKENS, QUERY_HEADS, HEAD_DIM), jnp.float32), -6.0, 6.0)
    return random_sample.astype(jnp.bfloat16)


def draw_prefix_keys(key, part):
    random_seed_key = jax.random.fold_in(key, 2)
    random_sample = jnp.clip(jax.random.normal(random_seed_key, (KEY_VALUE_HEADS, PREFIX_SLOTS, HEAD_DIM), jnp.float32), -6.0, 6.0)
    return random_sample.astype(jnp.bfloat16)


def with_ends(values, stream_key, smallest, high):
    longest = values.shape.index(max(values.shape))
    spots = []
    for shift in (0, 1):
        where = [jax.random.randint(jax.random.fold_in(stream_key, axis), (), 0, length) for axis, length in enumerate(values.shape)]
        where[longest] = (where[longest] + shift) % values.shape[longest]
        spots.append(tuple(where))
    return values.at[spots[0]].set(smallest).at[spots[1]].set(high)


def steps_of(key, shape, cuts, low, top_value):
    gain, own = 1.0, jax.random.fold_in(key, 6)
    for axis_at, parts in cuts:
        draws = jnp.exp(jax.random.uniform(jax.random.fold_in(own, axis_at), (parts,), jnp.float32, low / len(cuts), top_value / len(cuts)))
        gain = gain * jnp.repeat(draws, shape[axis_at] // parts).reshape([-1 if axis == axis_at else 1 for axis in range(len(shape))])
    return gain


def scatter_about(key, dims, width, most, shards=(), kind=jnp.bfloat16):
    loudness = steps_of(key, dims, shards, -0.22, 0.18) if shards else 1.0
    values = jax.random.normal(key, dims, jnp.float32) * width * loudness
    return jnp.minimum(jnp.maximum(values, -most), most).astype(kind)


def setup_inputs(seed: int = 0) -> dict:
    splits = jax.random.split(jax.random.key(seed), 7)
    queries = draw_queries(jax.random.fold_in(splits[6], 71), 0)
    prefix_keys = draw_prefix_keys(jax.random.fold_in(splits[6], 71), 0)
    cached_prefix_values = scatter_about(splits[2], (KEY_VALUE_HEADS, PREFIX_SLOTS, HEAD_DIM), 1.0, 6.0, ((0, 8), (1, 64)))
    shard_len = with_ends(jax.random.randint(splits[3], (SHARDS,), KEYS_DEV // 4, KEYS_DEV + 1), jax.random.fold_in(splits[3], 1), KEYS_DEV // 4, KEYS_DEV).astype(jnp.int32)
    reach = with_ends(jax.random.randint(splits[4], (SHARDS,), SPAN * KEYS_DEV // 2, SPAN * KEYS_DEV + 1), jax.random.fold_in(splits[4], 1), SPAN * KEYS_DEV // 2, SPAN * KEYS_DEV).astype(jnp.int32)
    w_out = scatter_about(splits[5], (QUERY_HEADS * HEAD_DIM, D), (QUERY_HEADS * HEAD_DIM) ** -0.5, 0.0625, ((0, 8), (1, 64)))
    return {"queries": queries, "prefix_keys": prefix_keys, "cached_prefix_values": cached_prefix_values, "shard_len": shard_len, "reach": reach, "w_out": w_out}


masked_score = -1e30


def part_stats(query_tile_rows, key_block, value_block, visible):
    scores = jnp.einsum("thgd,hnd->thgn", query_tile_rows.astype(jnp.float32), key_block.astype(jnp.float32)) * (HEAD_DIM ** -0.5)
    visible_grid = visible[:, None, None, :]
    maxima = jnp.max(jnp.where(visible_grid, scores, masked_score), axis=-1)
    weights = jnp.where(visible_grid, jnp.exp(scores - maxima[..., None]), 0.0)
    totals = jnp.sum(weights, axis=-1)
    weighted = jnp.einsum("thgn,hnd->thgd", weights.astype(jnp.bfloat16).astype(jnp.float32), value_block.astype(jnp.float32))
    return maxima, totals, weighted


def combine_parts(first, second):
    joined = jnp.maximum(first[0], second[0])
    first_factor = jnp.exp(first[0] - joined)
    second_factor = jnp.exp(second[0] - joined)
    totals = first[1] * first_factor + second[1] * second_factor
    weighted = first[2] * first_factor[..., None] + second[2] * second_factor[..., None]
    return joined, totals, weighted


def reference(queries, prefix_keys, cached_prefix_values, shard_len, reach, w_out):
    heads_per_group = QUERY_HEADS // KEY_VALUE_HEADS
    row_ids = jnp.arange(QUERY_TOKENS, dtype=jnp.int32)[:, None]
    slot_ids = jnp.arange(KEYS_DEV, dtype=jnp.int32)[None, :]

    def block_attention(block_id):
        starting_row = (block_id * QUERY_TOKENS).astype(jnp.int32)
        query_tile_rows = lax.dynamic_slice_in_dim(queries, starting_row, QUERY_TOKENS, 0).reshape(QUERY_TOKENS, KEY_VALUE_HEADS, heads_per_group, HEAD_DIM)
        running = None
        for offset in range(SPAN):
            shard_id = ((block_id + offset) % SHARDS).astype(jnp.int32)
            first_slot = (shard_id * KEYS_DEV).astype(jnp.int32)
            key_block = lax.dynamic_slice_in_dim(prefix_keys, first_slot, KEYS_DEV, 1)
            value_block = lax.dynamic_slice_in_dim(cached_prefix_values, first_slot, KEYS_DEV, 1)
            visible = (slot_ids < shard_len[shard_id]) & (offset * KEYS_DEV + slot_ids < reach[block_id] + row_ids)
            partial_value = part_stats(query_tile_rows, key_block, value_block, visible)
            running = partial_value if offset == 0 else combine_parts(running, partial_value)
        attended = (running[2] / running[1][..., None]).astype(jnp.bfloat16)
        return attended.reshape(QUERY_TOKENS, QUERY_HEADS * HEAD_DIM)

    attended = lax.map(block_attention, jnp.arange(SHARDS, dtype=jnp.int32)).reshape(TOKENS, QUERY_HEADS * HEAD_DIM)
    return jnp.dot(attended, w_out, preferred_element_type=jnp.float32).astype(jnp.bfloat16)
```

```python
import functools
import math

import jax
import jax.numpy as jnp
from jax import lax
from jax.experimental import pallas as pl
from jax.experimental.pallas import tpu as pltpu
from jax.sharding import Mesh
from jax.sharding import PartitionSpec as P

SPAN = 4
HEADS = ("y", "x")
BLK = ("Y", "Z", "K")
TILE = 128
NONE = -1e30
F32 = jnp.float32
BF16 = jnp.bfloat16


def eye_mask():
    rows = lax.broadcasted_iota(jnp.int32, (TILE, TILE), 0)
    lanes = lax.broadcasted_iota(jnp.int32, (TILE, TILE), 1)
    return rows == lanes


def attend_kernel(tokens, offset, lengths, reaches, q_ref, k_ref, v_ref, out_ref):
    rows, head_size = q_ref.shape
    count = lengths.shape[0]
    own_index = lax.axis_index(BLK)
    length = lengths[own_index]
    base = reaches[lax.rem(own_index + (count - offset), count)] - offset * k_ref.shape[0]
    scale = head_size**-0.5 * math.log2(math.e)
    eye = eye_mask()
    stats = []
    for start in range(0, rows, TILE):
        scores = lax.dot_general(
            q_ref[start : start + TILE, :],
            k_ref[...],
            (((1,), (1,)), ((), ())),
            preferred_element_type=F32,
        )
        row = start + lax.broadcasted_iota(jnp.int32, (TILE, 1), 0)
        limit = jnp.minimum(length, base + lax.rem(row, tokens))
        slot = lax.broadcasted_iota(jnp.int32, scores.shape, 1)
        scores = jnp.where(slot < limit, scores, NONE)
        top = jnp.max(scores, axis=1, keepdims=True)
        weights = jnp.exp2((scores - top) * scale)
        total = jnp.sum(weights, axis=1, keepdims=True)
        values = jnp.dot(weights.astype(BF16), v_ref[...], preferred_element_type=F32)
        seen = top > 0.1 * NONE
        out_ref[start : start + TILE, :] = jnp.where(seen, values / total, 0.0).astype(BF16)
        level = jnp.where(seen, top * scale + jnp.log2(total), NONE)
        spread = jnp.where(eye, jnp.broadcast_to(level, (TILE, TILE)), 0.0)
        stats.append(jnp.sum(spread, axis=0, keepdims=True))
    level = jnp.concatenate(stats, axis=0)
    high = level.astype(BF16).astype(F32)
    middle = (level - high).astype(BF16).astype(F32)
    low = level - high - middle
    out_ref[rows:, :] = jnp.concatenate(
        [high, middle, low, jnp.zeros_like(low)], axis=0
    ).astype(BF16)


def attend(tokens, offset, lengths, reaches, q, k, v):
    rows, head_size = q.shape
    slots = k.shape[0]
    extra = 4 * (rows // TILE)
    vmem = pl.BlockSpec(memory_space=pltpu.VMEM)
    return pl.pallas_call(
        functools.partial(attend_kernel, tokens, offset),
        out_shape=jax.ShapeDtypeStruct((rows + extra, head_size), BF16),
        in_specs=[pl.BlockSpec(memory_space=pltpu.SMEM)] * 2 + [vmem] * 3,
        out_specs=vmem,
        compiler_params=pltpu.CompilerParams(vmem_limit_bytes=24 << 20),
        cost_estimate=pl.CostEstimate(
            flops=4 * rows * slots * head_size,
            bytes_accessed=4 * slots * head_size,
            transcendentals=rows * slots,
        ),
        name="attend",
    )(lengths, reaches, q, k, v)


def combine_kernel(*refs):
    parts, out_ref = refs[:-1], refs[-1]
    copies, tokens, _ = out_ref.shape
    head_size = parts[0].shape[1]
    groups = parts[0].shape[0] // (TILE + 4)
    rows = groups * TILE
    levels = []
    for part in parts:
        terms = part[rows:, :].astype(F32)
        levels.append(
            terms[:groups] + terms[groups : 2 * groups] + terms[2 * groups : 3 * groups]
        )
    top = functools.reduce(jnp.maximum, levels)
    factors = [jnp.exp2(level - top) for level in levels]
    inverse = 1.0 / functools.reduce(jnp.add, factors)
    eye = eye_mask()
    per_tile = TILE // tokens
    for group in range(groups):
        total = None
        for part, factor in zip(parts, factors):
            line = jnp.broadcast_to((factor * inverse)[group : group + 1, :], (TILE, TILE))
            column = jnp.sum(jnp.where(eye, line, 0.0), axis=1, keepdims=True)
            term = part[group * TILE : (group + 1) * TILE, :].astype(F32) * column
            total = term if total is None else total + term
        total = total.astype(BF16)
        for i in range(per_tile):
            head = group * per_tile + i
            piece = total[i * tokens : (i + 1) * tokens]
            for copy in range(copies):
                out_ref[copy, :, head * head_size : (head + 1) * head_size] = piece


def combine(parts, copies, tokens, heads):
    head_size = parts[0].shape[1]
    vmem = pl.BlockSpec(memory_space=pltpu.VMEM)
    return pl.pallas_call(
        combine_kernel,
        out_shape=jax.ShapeDtypeStruct((copies, tokens, heads * head_size), BF16),
        in_specs=[vmem] * len(parts),
        out_specs=vmem,
        compiler_params=pltpu.CompilerParams(vmem_limit_bytes=8 << 20),
        cost_estimate=pl.CostEstimate(
            flops=1 << 20, bytes_accessed=1 << 20, transcendentals=0
        ),
        name="combine",
    )(*parts)


def project_kernel(own_ref, other_ref, w0, w1, w2, w3a, w3b, out_ref):
    columns = w0.shape[1]
    half = w3a.shape[0]
    lhs = jnp.concatenate([own_ref[0], other_ref[0]], axis=0)
    for i, w in enumerate((w0, w1, w2)):
        out_ref[0, :, i * columns : (i + 1) * columns] = jnp.dot(
            lhs, w[...], preferred_element_type=F32
        ).astype(BF16)
    last = jnp.dot(lhs[:, :half], w3a[...], preferred_element_type=F32)
    last += jnp.dot(lhs[:, half:], w3b[...], preferred_element_type=F32)
    out_ref[0, :, 3 * columns :] = last.astype(BF16)


def project(own, other, pieces):
    groups, rows, depth = own.shape
    columns = pieces[0].shape[1]
    whole = lambda w: pl.BlockSpec(w.shape, lambda i: (0, 0))
    side = pl.BlockSpec((1, rows, depth), lambda i: (i, 0, 0))
    return pl.pallas_call(
        project_kernel,
        grid=(groups,),
        out_shape=pltpu.HBM((groups, 2 * rows, 4 * columns), BF16),
        in_specs=[side, side] + [whole(w) for w in pieces],
        out_specs=pl.BlockSpec((1, 2 * rows, 4 * columns), lambda i: (i, 0, 0)),
        compiler_params=pltpu.CompilerParams(vmem_limit_bytes=24 << 20),
        cost_estimate=pl.CostEstimate(
            flops=16 * groups * rows * depth * columns,
            bytes_accessed=6 << 20,
            transcendentals=0,
        ),
        name="project",
    )(own, other, *pieces)


def total_kernel(place, in_ref, out_ref):
    half = out_ref.shape[1] // 2
    total = in_ref[0].astype(F32)
    for i in range(1, in_ref.shape[0]):
        total += in_ref[i].astype(F32)
    total = total.astype(BF16)
    core = place[4]
    out_ref[0, pl.ds(pl.multiple_of(core * half, half), half), :] = total[:half]
    out_ref[0, pl.ds(pl.multiple_of((1 - core) * half, half), half), :] = total[half:]


def totals(place, received, count):
    sources, rows, width = received.shape
    columns = width // count
    return pl.pallas_call(
        total_kernel,
        grid_spec=pltpu.PrefetchScalarGridSpec(
            num_scalar_prefetch=1,
            grid=(count,),
            in_specs=[pl.BlockSpec((sources, rows, columns), lambda i, place: (0, 0, i))],
            out_specs=pl.BlockSpec((1, rows, columns), lambda i, place: (place[i], 0, 0)),
        ),
        out_shape=jax.ShapeDtypeStruct((count, rows, columns), BF16),
        compiler_params=pltpu.CompilerParams(vmem_limit_bytes=16 << 20),
        cost_estimate=pl.CostEstimate(
            flops=sources * rows * width, bytes_accessed=3 << 20, transcendentals=0
        ),
        name="totals",
    )(place, received)


def passed_along(value, axis, steps):
    count = lax.axis_size(axis)
    return lax.ppermute(value, axis, [(i, (i + steps) % count) for i in range(count)])


def on_device(queries, prefix_keys, cached_prefix_values, shard_len, reach, w_out):
    shard_count = lax.axis_size(BLK)
    group_count = lax.axis_size(HEADS)
    y_count, z_count, k_count = (lax.axis_size(a) for a in BLK)
    tokens, heads, head_size = queries.shape
    depth, columns = w_out.shape
    per_group = shard_count // group_count
    keys = prefix_keys[0]
    values = cached_prefix_values[0]
    q_own = queries.transpose(1, 0, 2).reshape(heads * tokens, head_size)

    def home(block):
        slot = block % per_group
        return ((slot // k_count) * z_count + block // per_group) * k_count + slot % k_count

    visitors = [q_own]
    for j in range(1, SPAN):
        visitors.append(passed_along(q_own, BLK, j))
    half = depth // 2
    w_before = passed_along(w_out, "Y", 1)
    w_after = passed_along(w_out, "Y", -1)
    w_far_a = passed_along(w_before[:half], "Y", 1)
    w_far_b = passed_along(w_after[half:], "Y", -1)

    parts = []
    for j in range(SPAN):
        part = attend(tokens, j, shard_len, reach, visitors[j], keys, values)
        pairs = [(s, home((s - j) % shard_count)) for s in range(shard_count)]
        parts.append(lax.ppermute(part, BLK, pairs))
    spread = combine(parts, z_count, tokens, heads)
    own = lax.all_to_all(spread, "Z", split_axis=0, concat_axis=0, tiled=True)
    other = passed_along(own, "K", 1)
    partial = project(own, other, (w_out, w_before, w_after, w_far_a, w_far_b))
    received = lax.all_to_all(partial, HEADS, split_axis=0, concat_axis=0, tiled=True)
    y_index = lax.axis_index("Y")
    place = jnp.stack(
        [
            y_index,
            (y_index + y_count - 1) % y_count,
            (y_index + 1) % y_count,
            (y_index + 2) % y_count,
            lax.axis_index("K"),
        ]
    ).astype(jnp.int32)
    summed = totals(place, received, y_count)
    ordered = lax.all_to_all(summed, "Y", split_axis=0, concat_axis=0, tiled=True)
    return ordered.reshape(-1, columns)


def solution(mesh):
    finer = Mesh(mesh.devices.reshape(2, 4, 4, 8, 2), HEADS + BLK)
    placed = (
        P(BLK, HEADS, None),
        P(HEADS, BLK, None),
        P(HEADS, BLK, None),
        P(),
        P(),
        P(HEADS, BLK),
    )

    return jax.shard_map(
        on_device, mesh=finer, in_specs=placed, out_specs=P(HEADS, BLK), check_vma=False
    )
```

```python
import functools
import math

import jax
import jax.numpy as jnp
from jax import lax
from jax.experimental import pallas as pl
from jax.experimental.pallas import tpu as pltpu
from jax.sharding import Mesh
from jax.sharding import PartitionSpec as P

SPAN = 4
HEADS = ("y", "x")
BLK = ("Y", "Z", "K")
TILE = 128
NONE = -1e30
F32 = jnp.float32
BF16 = jnp.bfloat16


def eye_mask():
    rows = lax.broadcasted_iota(jnp.int32, (TILE, TILE), 0)
    lanes = lax.broadcasted_iota(jnp.int32, (TILE, TILE), 1)
    return rows == lanes


def part_body(offset, tokens, meta_ref, q_ref, k_ref, v_ref, out_ref):
    rows, head_size = q_ref.shape
    scale = head_size**-0.5 * math.log2(math.e)
    eye = eye_mask()
    length = meta_ref[SPAN : SPAN + 1, 0:1]
    base = meta_ref[offset : offset + 1, 0:1]
    stats = []
    for start in range(0, rows, TILE):
        scores = lax.dot_general(
            q_ref[start : start + TILE, :],
            k_ref[...],
            (((1,), (1,)), ((), ())),
            preferred_element_type=F32,
        )
        row = start + lax.broadcasted_iota(jnp.int32, (TILE, 1), 0)
        limit = jnp.minimum(length, base + row // (rows // tokens))
        slot = lax.broadcasted_iota(jnp.int32, scores.shape, 1)
        scores = jnp.where(slot < limit, scores, NONE)
        top = jnp.max(scores, axis=1, keepdims=True)
        weights = jnp.exp2((scores - top) * scale)
        total = jnp.sum(weights, axis=1, keepdims=True)
        values = jnp.dot(weights.astype(BF16), v_ref[...], preferred_element_type=F32)
        seen = top > 0.1 * NONE
        out_ref[start : start + TILE, :] = jnp.where(seen, values / total, 0.0).astype(BF16)
        level = jnp.where(seen, top * scale + jnp.log2(total), NONE)
        spread = jnp.where(eye, jnp.broadcast_to(level, (TILE, TILE)), 0.0)
        stats.append(jnp.sum(spread, axis=0, keepdims=True))
    level = jnp.concatenate(stats, axis=0)
    high = level.astype(BF16).astype(F32)
    middle = (level - high).astype(BF16).astype(F32)
    low = level - high - middle
    out_ref[rows:, :] = jnp.concatenate(
        [high, middle, low, jnp.zeros_like(low)], axis=0
    ).astype(BF16)


def first_kernel(tokens, *refs):
    out_ref, k_ref, v_ref, meta_ref, lengths, reaches, q_ref, sems = refs[5:]
    copies = [
        pltpu.make_async_copy(source, target, sems.at[i])
        for i, (source, target) in enumerate(zip(refs[:5], (lengths, reaches, q_ref, k_ref, v_ref)))
    ]
    for copy in copies:
        copy.start()
    copies[0].wait()
    copies[1].wait()
    count = lengths.shape[0]
    own_index = lax.axis_index(BLK)
    row = lax.broadcasted_iota(jnp.int32, meta_ref.shape, 0)
    meta = jnp.full(meta_ref.shape, lengths[own_index], jnp.int32)
    for j in range(SPAN):
        base = reaches[lax.rem(own_index + (count - j), count)] - j * k_ref.shape[0]
        meta = jnp.where(row == j, base, meta)
    meta_ref[...] = meta
    for copy in copies[2:]:
        copy.wait()
    part_body(0, tokens, meta_ref, q_ref, k_ref, v_ref, out_ref)


def part_cost(rows, slots, head_size):
    return pl.CostEstimate(
        flops=4 * rows * slots * head_size,
        bytes_accessed=4 * slots * head_size,
        transcendentals=rows * slots,
    )


VMEM = pl.BlockSpec(memory_space=pltpu.VMEM)


def first_part(tokens, lengths, reaches, q, k, v):
    rows, head_size = q.shape
    extra = 4 * (rows // TILE)
    hbm = pl.BlockSpec(memory_space=pltpu.HBM)
    return pl.pallas_call(
        functools.partial(first_kernel, tokens),
        out_shape=(
            jax.ShapeDtypeStruct((rows + extra, head_size), BF16),
            jax.ShapeDtypeStruct(k.shape, BF16),
            jax.ShapeDtypeStruct(v.shape, BF16),
            jax.ShapeDtypeStruct((8, 128), jnp.int32),
        ),
        in_specs=[hbm] * 5,
        out_specs=(VMEM,) * 4,
        scratch_shapes=[
            pltpu.SMEM(lengths.shape, jnp.int32),
            pltpu.SMEM(reaches.shape, jnp.int32),
            pltpu.VMEM(q.shape, BF16),
            pltpu.SemaphoreType.DMA((5,)),
        ],
        compiler_params=pltpu.CompilerParams(vmem_limit_bytes=24 << 20),
        cost_estimate=part_cost(rows, k.shape[0], head_size),
        name="first_part",
    )(*(pltpu.with_memory_space_constraint(a, pltpu.HBM) for a in (lengths, reaches, q, k, v)))


def later_part(tokens, offset, meta, q, k, v):
    rows, head_size = q.shape
    extra = 4 * (rows // TILE)
    return pl.pallas_call(
        functools.partial(part_body, offset, tokens),
        out_shape=jax.ShapeDtypeStruct((rows + extra, head_size), BF16),
        in_specs=[VMEM] * 4,
        out_specs=VMEM,
        compiler_params=pltpu.CompilerParams(vmem_limit_bytes=24 << 20),
        cost_estimate=part_cost(rows, k.shape[0], head_size),
        name="later_part",
    )(meta, q, k, v)


def combine_kernel(*refs):
    parts, out_ref, total_ref = refs[:-2], refs[-2], refs[-1]
    copies, tokens, _ = out_ref.shape
    head_size = parts[0].shape[1]
    groups = parts[0].shape[0] // (TILE + 4)
    rows = groups * TILE
    levels = []
    for part in parts:
        terms = part[rows:, :].astype(F32)
        levels.append(
            terms[:groups] + terms[groups : 2 * groups] + terms[2 * groups : 3 * groups]
        )
    top = functools.reduce(jnp.maximum, levels)
    factors = [jnp.exp2(level - top) for level in levels]
    inverse = 1.0 / functools.reduce(jnp.add, factors)
    eye = eye_mask()
    for group in range(groups):
        total = None
        for part, factor in zip(parts, factors):
            line = jnp.broadcast_to((factor * inverse)[group : group + 1, :], (TILE, TILE))
            column = jnp.sum(jnp.where(eye, line, 0.0), axis=1, keepdims=True)
            term = part[group * TILE : (group + 1) * TILE, :].astype(F32) * column
            total = term if total is None else total + term
        total_ref[group * TILE : (group + 1) * TILE, :] = total
    heads = rows // tokens
    for head in range(heads):
        piece = total_ref[pl.ds(head, tokens, stride=heads), :].astype(BF16)
        for copy in range(copies):
            out_ref[copy, :, head * head_size : (head + 1) * head_size] = piece


def combine(parts, copies, tokens, heads):
    head_size = parts[0].shape[1]
    vmem = pl.BlockSpec(memory_space=pltpu.VMEM)
    return pl.pallas_call(
        combine_kernel,
        out_shape=jax.ShapeDtypeStruct((copies, tokens, heads * head_size), BF16),
        in_specs=[vmem] * len(parts),
        out_specs=vmem,
        scratch_shapes=[pltpu.VMEM((heads * tokens, head_size), F32)],
        compiler_params=pltpu.CompilerParams(vmem_limit_bytes=8 << 20),
        cost_estimate=pl.CostEstimate(
            flops=1 << 20, bytes_accessed=1 << 20, transcendentals=0
        ),
        name="combine",
    )(*parts)


def project_kernel(own_ref, other_ref, w0, w1, w2, w3, out_ref):
    columns = w0.shape[1]
    lhs = jnp.concatenate([own_ref[0], other_ref[0]], axis=0)
    for i, w in enumerate((w0, w1, w2, w3)):
        out_ref[0, :, i * columns : (i + 1) * columns] = jnp.dot(
            lhs, w[...], preferred_element_type=F32
        ).astype(BF16)


def project(own, other, pieces):
    groups, rows, depth = own.shape
    columns = pieces[0].shape[1]
    half = groups // 2
    whole = lambda w: pl.BlockSpec(w.shape, lambda i: (0, 0))
    side = pl.BlockSpec((1, rows, depth), lambda i: ((i % 2) * half + i // 2, 0, 0))
    return pl.pallas_call(
        project_kernel,
        grid=(groups,),
        out_shape=pltpu.HBM((groups, 2 * rows, 4 * columns), BF16),
        in_specs=[side, side] + [whole(w) for w in pieces],
        out_specs=pl.BlockSpec((1, 2 * rows, 4 * columns), lambda i: (i, 0, 0)),
        compiler_params=pltpu.CompilerParams(vmem_limit_bytes=24 << 20),
        cost_estimate=pl.CostEstimate(
            flops=16 * groups * rows * depth * columns,
            bytes_accessed=6 << 20,
            transcendentals=0,
        ),
        name="project",
    )(own, other, *pieces)


def total_kernel(place, in_ref, *out_refs):
    half = in_ref.shape[1] // 2
    total = in_ref[0].astype(F32)
    for i in range(1, in_ref.shape[0]):
        total += in_ref[i].astype(F32)
    total = total.astype(BF16)
    core = lax.axis_index("K")
    for k, out_ref in enumerate(out_refs):

        @pl.when(pl.program_id(0) == k)
        def _():
            out_ref[pl.ds(pl.multiple_of(core * half, half), half), :] = total[:half]
            out_ref[pl.ds(pl.multiple_of((1 - core) * half, half), half), :] = total[half:]


def totals(place, received, count):
    sources, rows, width = received.shape
    columns = width // count
    return pl.pallas_call(
        total_kernel,
        grid_spec=pltpu.PrefetchScalarGridSpec(
            num_scalar_prefetch=1,
            grid=(count,),
            in_specs=[pl.BlockSpec((sources, rows, columns), lambda i, place: (0, 0, place[i]))],
            out_specs=[pl.BlockSpec((rows, columns), lambda i, place: (0, 0))] * count,
        ),
        out_shape=[jax.ShapeDtypeStruct((rows, columns), BF16)] * count,
        compiler_params=pltpu.CompilerParams(vmem_limit_bytes=16 << 20),
        cost_estimate=pl.CostEstimate(
            flops=sources * rows * width, bytes_accessed=3 << 20, transcendentals=0
        ),
        name="totals",
    )(place, received)


def order_kernel(*refs):
    pieces, out_ref = refs[:-1], refs[-1]
    count = len(pieces)
    rows = pieces[0].shape[0]
    own = lax.axis_index("Y")
    for k, piece in enumerate(pieces):
        slot = lax.rem(own + (count - k), count)
        out_ref[pl.ds(pl.multiple_of(slot * rows, rows), rows), :] = piece[...]


def in_order(pieces):
    rows, columns = pieces[0].shape
    return pl.pallas_call(
        order_kernel,
        out_shape=jax.ShapeDtypeStruct((len(pieces) * rows, columns), BF16),
        in_specs=[VMEM] * len(pieces),
        out_specs=VMEM,
        compiler_params=pltpu.CompilerParams(vmem_limit_bytes=4 << 20),
        cost_estimate=pl.CostEstimate(
            flops=1 << 18, bytes_accessed=1 << 19, transcendentals=0
        ),
        name="in_order",
    )(*pieces)


def passed_along(value, axis, steps):
    count = lax.axis_size(axis)
    return lax.ppermute(value, axis, [(i, (i + steps) % count) for i in range(count)])


def on_device(queries, prefix_keys, cached_prefix_values, shard_len, reach, w_out):
    y_count, z_count, _ = (lax.axis_size(a) for a in BLK)
    tokens, heads, head_size = queries.shape
    q_own = queries.reshape(tokens * heads, head_size)

    visitors = []
    for j in range(1, SPAN):
        visitors.append(passed_along(q_own, BLK, j))
    w_before = passed_along(w_out, "Y", 1)
    w_after = passed_along(w_out, "Y", -1)
    w_far = passed_along(w_out, "Y", 2)

    part, keys, values, meta = first_part(
        tokens, shard_len, reach, q_own, prefix_keys[0], cached_prefix_values[0]
    )
    parts = [part]
    for j in range(1, SPAN):
        part = later_part(tokens, j, meta, visitors[j - 1], keys, values)
        parts.append(passed_along(part, BLK, -j))
    spread = combine(parts, z_count, tokens, heads)
    own = lax.all_to_all(spread, "Z", split_axis=0, concat_axis=0, tiled=True)
    other = passed_along(own, "K", 1)
    partial = project(own, other, (w_out, w_before, w_after, w_far))
    received = lax.all_to_all(partial, HEADS, split_axis=0, concat_axis=0, tiled=True)
    x_half = lax.axis_size("x") // 2
    held = lax.axis_index("y") * x_half + lax.axis_index("x") // 2
    shift = (held + jnp.arange(y_count, dtype=jnp.int32) - lax.axis_index("Y")) % y_count
    place = jnp.where(shift == 0, 0, jnp.where(shift == y_count - 1, 1, shift + 1))
    summed = totals(place.astype(jnp.int32), received, y_count)
    moved = []
    for k in range(y_count):
        pairs = []
        for y in range(lax.axis_size("y")):
            for x in range(lax.axis_size("x")):
                for big in range(y_count):
                    target = (y * x_half + x // 2 + k) % y_count
                    group = (big // x_half) * 2 * x_half + (big % x_half) * 2 + x % 2
                    pairs.append(((y * 2 * x_half + x) * y_count + big, group * y_count + target))
        moved.append(lax.ppermute(summed[k], ("y", "x", "Y"), pairs))
    return in_order(moved)


def solution(mesh):
    finer = Mesh(mesh.devices.reshape(2, 4, 4, 8, 2), HEADS + BLK)
    placed = (
        P(BLK, HEADS, None),
        P(HEADS, BLK, None),
        P(HEADS, BLK, None),
        P(),
        P(),
        P(HEADS, BLK),
    )

    return jax.shard_map(
        on_device, mesh=finer, in_specs=placed, out_specs=P(HEADS, BLK), check_vma=False
    )
```

```python
import functools
import math

import jax
import jax.numpy as jnp
from jax import lax
from jax.experimental import pallas as pl
from jax.experimental.pallas import tpu as pltpu
from jax.sharding import Mesh
from jax.sharding import PartitionSpec as P

SPAN = 4
HEADS = ("y", "x")
BLK = ("Y", "Z", "K")
TILE = 128
NONE = -1e30
F32 = jnp.float32
BF16 = jnp.bfloat16


def eye_mask():
    rows = lax.broadcasted_iota(jnp.int32, (TILE, TILE), 0)
    lanes = lax.broadcasted_iota(jnp.int32, (TILE, TILE), 1)
    return rows == lanes


def part_body(offset, tokens, meta_ref, q_ref, k_ref, v_ref, out_ref):
    rows, head_size = q_ref.shape
    scale = head_size**-0.5 * math.log2(math.e)
    eye = eye_mask()
    length = meta_ref[SPAN : SPAN + 1, 0:1]
    base = meta_ref[offset : offset + 1, 0:1]
    stats = []
    for start in range(0, rows, TILE):
        scores = lax.dot_general(
            q_ref[start : start + TILE, :],
            k_ref[...],
            (((1,), (1,)), ((), ())),
            preferred_element_type=F32,
        )
        row = start + lax.broadcasted_iota(jnp.int32, (TILE, 1), 0)
        limit = jnp.minimum(length, base + row // (rows // tokens))
        slot = lax.broadcasted_iota(jnp.int32, scores.shape, 1)
        scores = jnp.where(slot < limit, scores, NONE)
        top = jnp.max(scores, axis=1, keepdims=True)
        weights = jnp.exp2((scores - top) * scale)
        total = jnp.sum(weights, axis=1, keepdims=True)
        values = jnp.dot(weights.astype(BF16), v_ref[...], preferred_element_type=F32)
        seen = top > 0.1 * NONE
        out_ref[start : start + TILE, :] = jnp.where(seen, values / total, 0.0).astype(BF16)
        level = jnp.where(seen, top * scale + jnp.log2(total), NONE)
        spread = jnp.where(eye, jnp.broadcast_to(level, (TILE, TILE)), 0.0)
        stats.append(jnp.sum(spread, axis=0, keepdims=True))
    level = jnp.concatenate(stats, axis=0)
    high = level.astype(BF16).astype(F32)
    middle = (level - high).astype(BF16).astype(F32)
    low = level - high - middle
    out_ref[rows:, :] = jnp.concatenate(
        [high, middle, low, jnp.zeros_like(low)], axis=0
    ).astype(BF16)


def first_kernel(tokens, *refs):
    out_ref, k_ref, v_ref, meta_ref, lengths, reaches, q_ref, sems = refs[5:]
    copies = [
        pltpu.make_async_copy(source, target, sems.at[i])
        for i, (source, target) in enumerate(zip(refs[:5], (lengths, reaches, q_ref, k_ref, v_ref)))
    ]
    for copy in copies:
        copy.start()
    copies[0].wait()
    copies[1].wait()
    count = lengths.shape[0]
    own_index = lax.axis_index(BLK)
    row = lax.broadcasted_iota(jnp.int32, meta_ref.shape, 0)
    meta = jnp.full(meta_ref.shape, lengths[own_index], jnp.int32)
    for j in range(SPAN):
        base = reaches[lax.rem(own_index + (count - j), count)] - j * k_ref.shape[0]
        meta = jnp.where(row == j, base, meta)
    meta_ref[...] = meta
    for copy in copies[2:]:
        copy.wait()
    part_body(0, tokens, meta_ref, q_ref, k_ref, v_ref, out_ref)


def part_cost(rows, slots, head_size):
    return pl.CostEstimate(
        flops=4 * rows * slots * head_size,
        bytes_accessed=4 * slots * head_size,
        transcendentals=rows * slots,
    )


VMEM = pl.BlockSpec(memory_space=pltpu.VMEM)


def first_part(tokens, lengths, reaches, q, k, v):
    rows, head_size = q.shape
    extra = 4 * (rows // TILE)
    hbm = pl.BlockSpec(memory_space=pltpu.HBM)
    return pl.pallas_call(
        functools.partial(first_kernel, tokens),
        out_shape=(
            jax.ShapeDtypeStruct((rows + extra, head_size), BF16),
            jax.ShapeDtypeStruct(k.shape, BF16),
            jax.ShapeDtypeStruct(v.shape, BF16),
            jax.ShapeDtypeStruct((8, 128), jnp.int32),
        ),
        in_specs=[hbm] * 5,
        out_specs=(VMEM,) * 4,
        scratch_shapes=[
            pltpu.SMEM(lengths.shape, jnp.int32),
            pltpu.SMEM(reaches.shape, jnp.int32),
            pltpu.VMEM(q.shape, BF16),
            pltpu.SemaphoreType.DMA((5,)),
        ],
        compiler_params=pltpu.CompilerParams(vmem_limit_bytes=24 << 20),
        cost_estimate=part_cost(rows, k.shape[0], head_size),
        name="first_part",
    )(*(pltpu.with_memory_space_constraint(a, pltpu.HBM) for a in (lengths, reaches, q, k, v)))


def later_part(tokens, offset, meta, q, k, v):
    rows, head_size = q.shape
    extra = 4 * (rows // TILE)
    return pl.pallas_call(
        functools.partial(part_body, offset, tokens),
        out_shape=jax.ShapeDtypeStruct((rows + extra, head_size), BF16),
        in_specs=[VMEM] * 4,
        out_specs=VMEM,
        compiler_params=pltpu.CompilerParams(vmem_limit_bytes=24 << 20),
        cost_estimate=part_cost(rows, k.shape[0], head_size),
        name="later_part",
    )(meta, q, k, v)


def combine_kernel(*refs):
    parts, out_ref, total_ref = refs[:-2], refs[-2], refs[-1]
    copies, tokens, _ = out_ref.shape
    head_size = parts[0].shape[1]
    groups = parts[0].shape[0] // (TILE + 4)
    rows = groups * TILE
    levels = []
    for part in parts:
        terms = part[rows:, :].astype(F32)
        levels.append(
            terms[:groups] + terms[groups : 2 * groups] + terms[2 * groups : 3 * groups]
        )
    top = functools.reduce(jnp.maximum, levels)
    factors = [jnp.exp2(level - top) for level in levels]
    inverse = 1.0 / functools.reduce(jnp.add, factors)
    eye = eye_mask()
    for group in range(groups):
        total = None
        for part, factor in zip(parts, factors):
            line = jnp.broadcast_to((factor * inverse)[group : group + 1, :], (TILE, TILE))
            column = jnp.sum(jnp.where(eye, line, 0.0), axis=1, keepdims=True)
            term = part[group * TILE : (group + 1) * TILE, :].astype(F32) * column
            total = term if total is None else total + term
        total_ref[group * TILE : (group + 1) * TILE, :] = total
    heads = rows // tokens
    for head in range(heads):
        piece = total_ref[pl.ds(head, tokens, stride=heads), :].astype(BF16)
        for copy in range(copies):
            out_ref[copy, :, head * head_size : (head + 1) * head_size] = piece


def combine(parts, copies, tokens, heads):
    head_size = parts[0].shape[1]
    vmem = pl.BlockSpec(memory_space=pltpu.VMEM)
    return pl.pallas_call(
        combine_kernel,
        out_shape=jax.ShapeDtypeStruct((copies, tokens, heads * head_size), BF16),
        in_specs=[vmem] * len(parts),
        out_specs=vmem,
        scratch_shapes=[pltpu.VMEM((heads * tokens, head_size), F32)],
        compiler_params=pltpu.CompilerParams(vmem_limit_bytes=8 << 20),
        cost_estimate=pl.CostEstimate(
            flops=1 << 20, bytes_accessed=1 << 20, transcendentals=0
        ),
        name="combine",
    )(*parts)


def project_kernel(own_ref, other_ref, w_ref, out_ref):
    rows = own_ref.shape[1]
    core = lax.axis_index("K")
    lhs = jnp.concatenate([own_ref[0], other_ref[0]], axis=0)
    for i in range(w_ref.shape[0]):
        part = jnp.dot(lhs, w_ref[i], preferred_element_type=F32).astype(BF16)
        out_ref[i, 0, pl.ds(pl.multiple_of(core * rows, rows), rows), :] = part[:rows]
        out_ref[i, 0, pl.ds(pl.multiple_of((1 - core) * rows, rows), rows), :] = part[rows:]


def project(own, other, weights, halves):
    groups, rows, depth = own.shape
    pieces, _, columns = weights.shape
    runs = groups // halves
    side = pl.BlockSpec((1, rows, depth), lambda i, j: (i * runs + j, 0, 0))
    return pl.pallas_call(
        project_kernel,
        grid=(halves, runs),
        out_shape=pltpu.HBM((pieces, halves, 2 * rows * runs, columns), BF16),
        in_specs=[side, side, pl.BlockSpec(weights.shape, lambda i, j: (0, 0, 0))],
        out_specs=pl.BlockSpec((pieces, 1, 2 * rows, columns), lambda i, j: (0, i, j, 0)),
        compiler_params=pltpu.CompilerParams(vmem_limit_bytes=24 << 20),
        cost_estimate=pl.CostEstimate(
            flops=4 * groups * rows * depth * columns * pieces,
            bytes_accessed=6 << 20,
            transcendentals=0,
        ),
        name="project",
    )(own, other, weights)


def total_kernel(in_ref, out_ref):
    total = in_ref[0].astype(F32)
    for i in range(1, in_ref.shape[0]):
        total += in_ref[i].astype(F32)
    out_ref[...] = total.astype(BF16)


def totals(received, steps):
    sources, rows, columns = received.shape
    step = rows // steps
    return pl.pallas_call(
        total_kernel,
        grid=(steps,),
        out_shape=jax.ShapeDtypeStruct((rows, columns), BF16),
        in_specs=[pl.BlockSpec((sources, step, columns), lambda i: (0, i, 0))],
        out_specs=pl.BlockSpec((step, columns), lambda i: (i, 0)),
        compiler_params=pltpu.CompilerParams(vmem_limit_bytes=16 << 20),
        cost_estimate=pl.CostEstimate(
            flops=sources * rows * columns, bytes_accessed=3 << 20, transcendentals=0
        ),
        name="totals",
    )(received)


def passed_along(value, axis, steps):
    count = lax.axis_size(axis)
    return lax.ppermute(value, axis, [(i, (i + steps) % count) for i in range(count)])


def on_device(queries, prefix_keys, cached_prefix_values, shard_len, reach, w_out):
    y_count, z_count = lax.axis_size("Y"), lax.axis_size("Z")
    tokens, heads, head_size = queries.shape
    q_own = queries.reshape(tokens * heads, head_size)

    visitors = []
    for j in range(1, SPAN):
        visitors.append(passed_along(q_own, BLK, j))
    weights = lax.all_gather(w_out, "Y", axis=0, tiled=False)

    part, keys, values, meta = first_part(
        tokens, shard_len, reach, q_own, prefix_keys[0], cached_prefix_values[0]
    )
    parts = [part]
    for j in range(1, SPAN):
        part = later_part(tokens, j, meta, visitors[j - 1], keys, values)
        parts.append(passed_along(part, BLK, -j))
    spread = combine(parts, z_count, tokens, heads)
    own = lax.all_to_all(spread, "Z", split_axis=0, concat_axis=0, tiled=True)
    other = passed_along(own, "K", 1)
    x_half = lax.axis_size("x") // 2
    partial = project(own, other, weights, 2)
    partial = partial.reshape(-1, *partial.shape[2:])
    received = lax.all_to_all(partial, HEADS, split_axis=0, concat_axis=0, tiled=True)
    summed = totals(received, 4)
    pairs = []
    for y in range(lax.axis_size("y")):
        for x in range(lax.axis_size("x")):
            for big in range(y_count):
                head = (big // x_half) * 2 * x_half + (big % x_half) * 2 + x % 2
                target = head * y_count + y * x_half + x // 2
                pairs.append(((y * 2 * x_half + x) * y_count + big, target))
    return lax.ppermute(summed, ("y", "x", "Y"), pairs)


def solution(mesh):
    finer = Mesh(mesh.devices.reshape(2, 4, 4, 8, 2), HEADS + BLK)
    placed = (
        P(BLK, HEADS, None),
        P(HEADS, BLK, None),
        P(HEADS, BLK, None),
        P(),
        P(),
        P(HEADS, BLK),
    )

    return jax.shard_map(
        on_device, mesh=finer, in_specs=placed, out_specs=P(HEADS, BLK), check_vma=False
    )
```

```python
import functools
import math

import jax
import jax.numpy as jnp
from jax import lax
from jax.experimental import pallas as pl
from jax.experimental.pallas import tpu as pltpu
from jax.sharding import Mesh
from jax.sharding import PartitionSpec as P

HEADS = ("y", "x")
BLK = ("Y", "Z", "K")
TILE = 128
NONE = -1e30
F32 = jnp.float32
BF16 = jnp.bfloat16


def eye_mask():
    rows = lax.broadcasted_iota(jnp.int32, (TILE, TILE), 0)
    lanes = lax.broadcasted_iota(jnp.int32, (TILE, TILE), 1)
    return rows == lanes


def part_body(q_ref, shards, out_ref, tokens):
    rows, head_size = q_ref.shape
    scale = head_size**-0.5 * math.log2(math.e)
    eye = eye_mask()
    stats = []
    for start in range(0, rows, TILE):
        row = start + lax.broadcasted_iota(jnp.int32, (TILE, 1), 0)
        scored = []
        for k_ref, _, length, base in shards:
            scores = lax.dot_general(
                q_ref[start : start + TILE, :],
                k_ref[...],
                (((1,), (1,)), ((), ())),
                preferred_element_type=F32,
            )
            limit = jnp.minimum(length, base + row // (rows // tokens))
            slot = lax.broadcasted_iota(jnp.int32, scores.shape, 1)
            scored.append(jnp.where(slot < limit, scores, NONE))
        top = functools.reduce(
            jnp.maximum, [jnp.max(scores, axis=1, keepdims=True) for scores in scored]
        )
        total, values = 0.0, 0.0
        for scores, (_, v_ref, _, _) in zip(scored, shards):
            weights = jnp.exp2((scores - top) * scale)
            total += jnp.sum(weights, axis=1, keepdims=True)
            values += jnp.dot(weights.astype(BF16), v_ref[...], preferred_element_type=F32)
        seen = top > 0.1 * NONE
        out_ref[start : start + TILE, :] = jnp.where(seen, values / total, 0.0).astype(BF16)
        level = jnp.where(seen, top * scale + jnp.log2(total), NONE)
        spread = jnp.where(eye, jnp.broadcast_to(level, (TILE, TILE)), 0.0)
        stats.append(jnp.sum(spread, axis=0, keepdims=True))
    level = jnp.concatenate(stats, axis=0)
    high = level.astype(BF16).astype(F32)
    middle = (level - high).astype(BF16).astype(F32)
    low = level - high - middle
    out_ref[rows:, :] = jnp.concatenate(
        [high, middle, low, jnp.zeros_like(low)], axis=0
    ).astype(BF16)


def known(meta_ref, i):
    return meta_ref[i : i + 1, 0:1]


def first_kernel(tokens, *refs):
    out_ref, k_ref, v_ref, meta_ref, lengths, reaches, q_ref, sems = refs[5:]
    copies = [
        pltpu.make_async_copy(source, target, sems.at[i])
        for i, (source, target) in enumerate(zip(refs[:5], (lengths, reaches, q_ref, k_ref, v_ref)))
    ]
    for copy in copies:
        copy.start()
    copies[0].wait()
    copies[1].wait()
    count = lengths.shape[0]
    slots = k_ref.shape[0]
    own = lax.axis_index(BLK)
    core = lax.axis_index("K")
    reach = lambda back: reaches[lax.rem(own + (count - back), count)]
    facts = (
        lengths[own],
        lengths[own + 1 - 2 * core],
        reach(0),
        reach(2) - 2 * slots,
        reach(2) - (3 - 2 * core) * slots,
        reach(4 * core) - (1 + 2 * core) * slots,
    )
    row = lax.broadcasted_iota(jnp.int32, meta_ref.shape, 0)
    meta = jnp.zeros(meta_ref.shape, jnp.int32)
    for i, fact in enumerate(facts):
        meta = jnp.where(row == i, fact, meta)
    meta_ref[...] = meta
    for copy in copies[2:]:
        copy.wait()
    part_body(q_ref, [(k_ref, v_ref, known(meta_ref, 0), known(meta_ref, 2))], out_ref, tokens)


def second_kernel(tokens, meta_ref, q_ref, k_ref, v_ref, k_other, v_other, out_ref):
    shards = [
        (k_ref, v_ref, known(meta_ref, 0), known(meta_ref, 3)),
        (k_other, v_other, known(meta_ref, 1), known(meta_ref, 4)),
    ]
    part_body(q_ref, shards, out_ref, tokens)


def third_kernel(tokens, meta_ref, q_own, q_visit, k_other, v_other, out_ref, q_ref):
    q_ref[...] = jnp.where(lax.axis_index("K") == 0, q_own[...], q_visit[...])
    shards = [(k_other, v_other, known(meta_ref, 1), known(meta_ref, 5))]
    part_body(q_ref, shards, out_ref, tokens)


def part_cost(rows, slots, head_size):
    return pl.CostEstimate(
        flops=4 * rows * slots * head_size,
        bytes_accessed=4 * slots * head_size,
        transcendentals=rows * slots,
    )


VMEM = pl.BlockSpec(memory_space=pltpu.VMEM)


def first_part(tokens, lengths, reaches, q, k, v):
    rows, head_size = q.shape
    extra = 4 * (rows // TILE)
    hbm = pl.BlockSpec(memory_space=pltpu.HBM)
    return pl.pallas_call(
        functools.partial(first_kernel, tokens),
        out_shape=(
            jax.ShapeDtypeStruct((rows + extra, head_size), BF16),
            jax.ShapeDtypeStruct(k.shape, BF16),
            jax.ShapeDtypeStruct(v.shape, BF16),
            jax.ShapeDtypeStruct((8, 128), jnp.int32),
        ),
        in_specs=[hbm] * 5,
        out_specs=(VMEM,) * 4,
        scratch_shapes=[
            pltpu.SMEM(lengths.shape, jnp.int32),
            pltpu.SMEM(reaches.shape, jnp.int32),
            pltpu.VMEM(q.shape, BF16),
            pltpu.SemaphoreType.DMA((5,)),
        ],
        compiler_params=pltpu.CompilerParams(vmem_limit_bytes=24 << 20),
        cost_estimate=part_cost(rows, k.shape[0], head_size),
        name="first_part",
    )(*(pltpu.with_memory_space_constraint(a, pltpu.HBM) for a in (lengths, reaches, q, k, v)))


def later_part(kernel, tokens, slots, scratch, *arrays):
    rows, head_size = arrays[1].shape
    extra = 4 * (rows // TILE)
    return pl.pallas_call(
        functools.partial(kernel, tokens),
        out_shape=jax.ShapeDtypeStruct((rows + extra, head_size), BF16),
        in_specs=[VMEM] * len(arrays),
        out_specs=VMEM,
        scratch_shapes=scratch,
        compiler_params=pltpu.CompilerParams(vmem_limit_bytes=24 << 20),
        cost_estimate=part_cost(rows, slots, head_size),
    )(*arrays)


def combine_kernel(*refs):
    parts, out_ref, total_ref = refs[:-2], refs[-2], refs[-1]
    copies, tokens, _ = out_ref.shape
    head_size = parts[0].shape[1]
    groups = parts[0].shape[0] // (TILE + 4)
    rows = groups * TILE
    south = lax.axis_index("K") == 0

    def taken(part, start, stop):
        if isinstance(part, tuple):
            return jnp.where(south, part[0][start:stop, :], part[1][start:stop, :])
        return part[start:stop, :]

    parts = list(parts[:-2]) + [tuple(parts[-2:])]
    levels = []
    for part in parts:
        terms = taken(part, rows, rows + 4 * groups).astype(F32)
        levels.append(
            terms[:groups] + terms[groups : 2 * groups] + terms[2 * groups : 3 * groups]
        )
    top = functools.reduce(jnp.maximum, levels)
    factors = [jnp.exp2(level - top) for level in levels]
    inverse = 1.0 / functools.reduce(jnp.add, factors)
    eye = eye_mask()
    for group in range(groups):
        total = None
        for part, factor in zip(parts, factors):
            line = jnp.broadcast_to((factor * inverse)[group : group + 1, :], (TILE, TILE))
            column = jnp.sum(jnp.where(eye, line, 0.0), axis=1, keepdims=True)
            term = taken(part, group * TILE, (group + 1) * TILE).astype(F32) * column
            total = term if total is None else total + term
        total_ref[group * TILE : (group + 1) * TILE, :] = total
    heads = rows // tokens
    for head in range(heads):
        piece = total_ref[pl.ds(head, tokens, stride=heads), :].astype(BF16)
        for copy in range(copies):
            out_ref[copy, :, head * head_size : (head + 1) * head_size] = piece


def combine(parts, copies, tokens, heads):
    head_size = parts[0].shape[1]
    vmem = pl.BlockSpec(memory_space=pltpu.VMEM)
    return pl.pallas_call(
        combine_kernel,
        out_shape=jax.ShapeDtypeStruct((copies, tokens, heads * head_size), BF16),
        in_specs=[vmem] * len(parts),
        out_specs=vmem,
        scratch_shapes=[pltpu.VMEM((heads * tokens, head_size), F32)],
        compiler_params=pltpu.CompilerParams(vmem_limit_bytes=8 << 20),
        cost_estimate=pl.CostEstimate(
            flops=1 << 20, bytes_accessed=1 << 20, transcendentals=0
        ),
        name="combine",
    )(*parts)


def project_kernel(side_ref, w_ref, out_ref):
    count, rows, depth = side_ref.shape
    lhs = side_ref[...].reshape(count * rows, depth)
    for i in range(w_ref.shape[0]):
        out_ref[i, 0] = jnp.dot(lhs, w_ref[i], preferred_element_type=F32).astype(BF16)


def project(side, weights, halves):
    groups, rows, depth = side.shape
    pieces, _, columns = weights.shape
    runs = groups // halves
    return pl.pallas_call(
        project_kernel,
        grid=(halves, runs // 2),
        out_shape=pltpu.HBM((pieces, halves, rows * runs, columns), BF16),
        in_specs=[
            pl.BlockSpec((2, rows, depth), lambda i, j: (i * (runs // 2) + j, 0, 0)),
            pl.BlockSpec(weights.shape, lambda i, j: (0, 0, 0)),
        ],
        out_specs=pl.BlockSpec((pieces, 1, 2 * rows, columns), lambda i, j: (0, i, j, 0)),
        compiler_params=pltpu.CompilerParams(vmem_limit_bytes=24 << 20),
        cost_estimate=pl.CostEstimate(
            flops=2 * groups * rows * depth * columns * pieces,
            bytes_accessed=4 << 20,
            transcendentals=0,
        ),
        name="project",
    )(side, weights)


def total_kernel(in_ref, out_ref):
    total = in_ref[0].astype(F32)
    for i in range(1, in_ref.shape[0]):
        total += in_ref[i].astype(F32)
    out_ref[...] = total.astype(BF16)


def totals(received, steps):
    sources, rows, columns = received.shape
    step = rows // steps
    return pl.pallas_call(
        total_kernel,
        grid=(steps,),
        out_shape=jax.ShapeDtypeStruct((rows, columns), BF16),
        in_specs=[pl.BlockSpec((sources, step, columns), lambda i: (0, i, 0))],
        out_specs=pl.BlockSpec((step, columns), lambda i: (i, 0)),
        compiler_params=pltpu.CompilerParams(vmem_limit_bytes=16 << 20),
        cost_estimate=pl.CostEstimate(
            flops=sources * rows * columns, bytes_accessed=3 << 20, transcendentals=0
        ),
        name="totals",
    )(received)


def order_kernel(runs, own_ref, other_ref, out_ref):
    rows = own_ref.shape[0] // runs
    core = lax.axis_index("K")
    for i in range(runs):
        for ref, slot in ((own_ref, core), (other_ref, 1 - core)):
            start = pl.multiple_of(slot * rows + 2 * i * rows, rows)
            out_ref[pl.ds(start, rows), :] = ref[i * rows : (i + 1) * rows, :]


def in_order(runs, own, other):
    rows, columns = own.shape
    return pl.pallas_call(
        functools.partial(order_kernel, runs),
        out_shape=jax.ShapeDtypeStruct((2 * rows, columns), BF16),
        in_specs=[VMEM] * 2,
        out_specs=VMEM,
        compiler_params=pltpu.CompilerParams(vmem_limit_bytes=4 << 20),
        cost_estimate=pl.CostEstimate(
            flops=1 << 18, bytes_accessed=1 << 19, transcendentals=0
        ),
        name="in_order",
    )(own, other)


def passed_along(value, axis, steps):
    count = lax.axis_size(axis)
    return lax.ppermute(value, axis, [(i, (i + steps) % count) for i in range(count)])


def on_device(queries, prefix_keys, cached_prefix_values, shard_len, reach, w_out):
    y_count, z_count = lax.axis_size("Y"), lax.axis_size("Z")
    shard_count = lax.axis_size(BLK)
    tokens, heads, head_size = queries.shape
    q_own = queries.reshape(tokens * heads, head_size)
    slots = prefix_keys.shape[1]
    odd = range(1, shard_count, 2)
    q_near = passed_along(q_own, BLK, 2)
    q_far = lax.ppermute(q_own, BLK, [(i, (i + 4) % shard_count) for i in odd])
    k_other = passed_along(prefix_keys[0], "K", 1)
    v_other = passed_along(cached_prefix_values[0], "K", 1)
    weights = lax.all_gather(w_out, "Y", axis=0, tiled=False)

    part_own, keys, values, meta = first_part(
        tokens, shard_len, reach, q_own, prefix_keys[0], cached_prefix_values[0]
    )
    part_near = later_part(
        second_kernel, tokens, 2 * slots, [],
        meta, q_near, keys, values, k_other, v_other,
    )
    back_near = passed_along(part_near, BLK, -2)
    part_far = later_part(
        third_kernel, tokens, slots, [pltpu.VMEM(q_own.shape, BF16)],
        meta, q_own, q_far, k_other, v_other,
    )
    back_far = lax.ppermute(part_far, BLK, [(i, (i - 4) % shard_count) for i in odd])
    spread = combine([part_own, back_near, part_far, back_far], z_count, tokens, heads)
    own = lax.all_to_all(spread, "Z", split_axis=0, concat_axis=0, tiled=True)
    other = passed_along(own, "K", 1)
    x_half = lax.axis_size("x") // 2
    pairs = []
    for y in range(lax.axis_size("y")):
        for x in range(lax.axis_size("x")):
            for big in range(y_count):
                head = (big // x_half) * 2 * x_half + (big % x_half) * 2 + x % 2
                target = head * y_count + y * x_half + x // 2
                pairs.append(((y * 2 * x_half + x) * y_count + big, target))
    placed = []
    for side in (own, other):
        partial = project(side, weights, 2)
        partial = partial.reshape(-1, *partial.shape[2:])
        received = lax.all_to_all(partial, HEADS, split_axis=0, concat_axis=0, tiled=True)
        summed = totals(received, 2)
        placed.append(lax.ppermute(summed, ("y", "x", "Y"), pairs))
    return in_order(z_count // 2, *placed)


def solution(mesh):
    finer = Mesh(mesh.devices.reshape(2, 4, 4, 8, 2), HEADS + BLK)
    placed = (
        P(BLK, HEADS, None),
        P(HEADS, BLK, None),
        P(HEADS, BLK, None),
        P(),
        P(),
        P(HEADS, BLK),
    )

    return jax.shard_map(
        on_device, mesh=finer, in_specs=placed, out_specs=P(HEADS, BLK), check_vma=False
    )
```

```python
import functools
import math

import jax
import jax.numpy as jnp
from jax import lax
from jax.experimental import pallas as pl
from jax.experimental.pallas import tpu as pltpu
from jax.sharding import Mesh
from jax.sharding import PartitionSpec as P

HEADS = ("y", "x")
BLK = ("Y", "Z", "K")
TILE = 128
NONE = -1e30
F32 = jnp.float32
BF16 = jnp.bfloat16


def eye_mask():
    rows = lax.broadcasted_iota(jnp.int32, (TILE, TILE), 0)
    lanes = lax.broadcasted_iota(jnp.int32, (TILE, TILE), 1)
    return rows == lanes


def part_body(q_ref, shards, out_ref, tokens):
    rows, head_size = q_ref.shape
    scale = head_size**-0.5 * math.log2(math.e)
    eye = eye_mask()
    stats = []
    for start in range(0, rows, TILE):
        row = start + lax.broadcasted_iota(jnp.int32, (TILE, 1), 0)
        scored = []
        for k_ref, _, length, base in shards:
            scores = lax.dot_general(
                q_ref[start : start + TILE, :],
                k_ref[...],
                (((1,), (1,)), ((), ())),
                preferred_element_type=F32,
            )
            limit = jnp.minimum(length, base + row // (rows // tokens))
            slot = lax.broadcasted_iota(jnp.int32, scores.shape, 1)
            scored.append(jnp.where(slot < limit, scores, NONE))
        top = functools.reduce(
            jnp.maximum, [jnp.max(scores, axis=1, keepdims=True) for scores in scored]
        )
        total, values = 0.0, 0.0
        for scores, (_, v_ref, _, _) in zip(scored, shards):
            weights = jnp.exp2((scores - top) * scale)
            total += jnp.sum(weights, axis=1, keepdims=True)
            values += jnp.dot(weights.astype(BF16), v_ref[...], preferred_element_type=F32)
        seen = top > 0.1 * NONE
        out_ref[start : start + TILE, :] = jnp.where(seen, values / total, 0.0).astype(BF16)
        level = jnp.where(seen, top * scale + jnp.log2(total), NONE)
        spread = jnp.where(eye, jnp.broadcast_to(level, (TILE, TILE)), 0.0)
        stats.append(jnp.sum(spread, axis=0, keepdims=True))
    level = jnp.concatenate(stats, axis=0)
    high = level.astype(BF16).astype(F32)
    middle = (level - high).astype(BF16).astype(F32)
    low = level - high - middle
    out_ref[rows:, :] = jnp.concatenate(
        [high, middle, low, jnp.zeros_like(low)], axis=0
    ).astype(BF16)


def known(meta_ref, i):
    return meta_ref[i : i + 1, 0:1]


def first_kernel(tokens, *refs):
    out_ref, k_ref, v_ref, meta_ref, lengths, reaches, q_ref, sems = refs[5:]
    copies = [
        pltpu.make_async_copy(source, target, sems.at[i])
        for i, (source, target) in enumerate(zip(refs[:5], (lengths, reaches, q_ref, k_ref, v_ref)))
    ]
    for copy in copies:
        copy.start()
    copies[0].wait()
    copies[1].wait()
    count = lengths.shape[0]
    slots = k_ref.shape[0]
    own = lax.axis_index(BLK)
    core = lax.axis_index("K")
    reach = lambda back: reaches[lax.rem(own + (count - back), count)]
    facts = (
        lengths[own],
        lengths[own + 1 - 2 * core],
        reach(0),
        reach(2) - 2 * slots,
        reach(2) - (3 - 2 * core) * slots,
        reach(4 * core) - (1 + 2 * core) * slots,
    )
    row = lax.broadcasted_iota(jnp.int32, meta_ref.shape, 0)
    meta = jnp.zeros(meta_ref.shape, jnp.int32)
    for i, fact in enumerate(facts):
        meta = jnp.where(row == i, fact, meta)
    meta_ref[...] = meta
    for copy in copies[2:]:
        copy.wait()
    part_body(q_ref, [(k_ref, v_ref, known(meta_ref, 0), known(meta_ref, 2))], out_ref, tokens)


def second_kernel(tokens, meta_ref, q_ref, k_ref, v_ref, k_other, v_other, out_ref):
    shards = [
        (k_ref, v_ref, known(meta_ref, 0), known(meta_ref, 3)),
        (k_other, v_other, known(meta_ref, 1), known(meta_ref, 4)),
    ]
    part_body(q_ref, shards, out_ref, tokens)


def third_kernel(tokens, meta_ref, q_own, q_visit, k_other, v_other, out_ref, q_ref):
    q_ref[...] = jnp.where(lax.axis_index("K") == 0, q_own[...], q_visit[...])
    shards = [(k_other, v_other, known(meta_ref, 1), known(meta_ref, 5))]
    part_body(q_ref, shards, out_ref, tokens)


def part_cost(rows, slots, head_size):
    return pl.CostEstimate(
        flops=4 * rows * slots * head_size,
        bytes_accessed=4 * slots * head_size,
        transcendentals=rows * slots,
    )


VMEM = pl.BlockSpec(memory_space=pltpu.VMEM)


def first_part(tokens, lengths, reaches, q, k, v):
    rows, head_size = q.shape
    extra = 4 * (rows // TILE)
    hbm = pl.BlockSpec(memory_space=pltpu.HBM)
    return pl.pallas_call(
        functools.partial(first_kernel, tokens),
        out_shape=(
            jax.ShapeDtypeStruct((rows + extra, head_size), BF16),
            jax.ShapeDtypeStruct(k.shape, BF16),
            jax.ShapeDtypeStruct(v.shape, BF16),
            jax.ShapeDtypeStruct((8, 128), jnp.int32),
        ),
        in_specs=[hbm] * 5,
        out_specs=(VMEM,) * 4,
        scratch_shapes=[
            pltpu.SMEM(lengths.shape, jnp.int32),
            pltpu.SMEM(reaches.shape, jnp.int32),
            pltpu.VMEM(q.shape, BF16),
            pltpu.SemaphoreType.DMA((5,)),
        ],
        compiler_params=pltpu.CompilerParams(vmem_limit_bytes=24 << 20),
        cost_estimate=part_cost(rows, k.shape[0], head_size),
        name="first_part",
    )(*(pltpu.with_memory_space_constraint(a, pltpu.HBM) for a in (lengths, reaches, q, k, v)))


def later_part(kernel, tokens, slots, scratch, *arrays):
    rows, head_size = arrays[1].shape
    extra = 4 * (rows // TILE)
    return pl.pallas_call(
        functools.partial(kernel, tokens),
        out_shape=jax.ShapeDtypeStruct((rows + extra, head_size), BF16),
        in_specs=[VMEM] * len(arrays),
        out_specs=VMEM,
        scratch_shapes=scratch,
        compiler_params=pltpu.CompilerParams(vmem_limit_bytes=24 << 20),
        cost_estimate=part_cost(rows, slots, head_size),
    )(*arrays)


def combine_kernel(*refs):
    parts, out_ref, total_ref = refs[:-2], refs[-2], refs[-1]
    copies, tokens, _ = out_ref.shape
    head_size = parts[0].shape[1]
    groups = parts[0].shape[0] // (TILE + 4)
    rows = groups * TILE
    south = lax.axis_index("K") == 0

    def taken(part, start, stop):
        if isinstance(part, tuple):
            return jnp.where(south, part[0][start:stop, :], part[1][start:stop, :])
        return part[start:stop, :]

    parts = list(parts[:-2]) + [tuple(parts[-2:])]
    levels = []
    for part in parts:
        terms = taken(part, rows, rows + 4 * groups).astype(F32)
        levels.append(
            terms[:groups] + terms[groups : 2 * groups] + terms[2 * groups : 3 * groups]
        )
    top = functools.reduce(jnp.maximum, levels)
    factors = [jnp.exp2(level - top) for level in levels]
    inverse = 1.0 / functools.reduce(jnp.add, factors)
    eye = eye_mask()
    for group in range(groups):
        total = None
        for part, factor in zip(parts, factors):
            line = jnp.broadcast_to((factor * inverse)[group : group + 1, :], (TILE, TILE))
            column = jnp.sum(jnp.where(eye, line, 0.0), axis=1, keepdims=True)
            term = taken(part, group * TILE, (group + 1) * TILE).astype(F32) * column
            total = term if total is None else total + term
        total_ref[group * TILE : (group + 1) * TILE, :] = total
    heads = rows // tokens
    for head in range(heads):
        piece = total_ref[pl.ds(head, tokens, stride=heads), :].astype(BF16)
        for copy in range(copies):
            out_ref[copy, :, head * head_size : (head + 1) * head_size] = piece


def combine(parts, copies, tokens, heads):
    head_size = parts[0].shape[1]
    vmem = pl.BlockSpec(memory_space=pltpu.VMEM)
    return pl.pallas_call(
        combine_kernel,
        out_shape=jax.ShapeDtypeStruct((copies, tokens, heads * head_size), BF16),
        in_specs=[vmem] * len(parts),
        out_specs=vmem,
        scratch_shapes=[pltpu.VMEM((heads * tokens, head_size), F32)],
        compiler_params=pltpu.CompilerParams(vmem_limit_bytes=8 << 20),
        cost_estimate=pl.CostEstimate(
            flops=1 << 20, bytes_accessed=1 << 20, transcendentals=0
        ),
        name="combine",
    )(*parts)


def project_kernel(side_ref, w_ref, out_ref):
    count, rows, depth = side_ref.shape
    lhs = side_ref[...].reshape(count * rows, depth)
    part = jnp.dot(lhs, w_ref[0], preferred_element_type=F32).astype(BF16)
    out_ref[...] = part.reshape(out_ref.shape)


def project(side, weights, halves):
    groups, rows, depth = side.shape
    pieces, _, columns = weights.shape
    runs = groups // halves
    return pl.pallas_call(
        project_kernel,
        grid=(pieces,),
        out_shape=pltpu.HBM((pieces, halves, rows * runs, columns), BF16),
        in_specs=[
            pl.BlockSpec((groups, rows, depth), lambda i: (0, 0, 0)),
            pl.BlockSpec((1, depth, columns), lambda i: (i, 0, 0)),
        ],
        out_specs=pl.BlockSpec((1, halves, rows * runs, columns), lambda i: (i, 0, 0, 0)),
        compiler_params=pltpu.CompilerParams(vmem_limit_bytes=24 << 20),
        cost_estimate=pl.CostEstimate(
            flops=2 * groups * rows * depth * columns * pieces,
            bytes_accessed=4 << 20,
            transcendentals=0,
        ),
        name="project",
    )(side, pltpu.with_memory_space_constraint(weights, pltpu.HBM))


def total_kernel(in_ref, out_ref):
    total = in_ref[0].astype(F32)
    for i in range(1, in_ref.shape[0]):
        total += in_ref[i].astype(F32)
    out_ref[...] = total.astype(BF16)


def totals(received, steps):
    sources, rows, columns = received.shape
    step = rows // steps
    return pl.pallas_call(
        total_kernel,
        grid=(steps,),
        out_shape=jax.ShapeDtypeStruct((rows, columns), BF16),
        in_specs=[pl.BlockSpec((sources, step, columns), lambda i: (0, i, 0))],
        out_specs=pl.BlockSpec((step, columns), lambda i: (i, 0)),
        compiler_params=pltpu.CompilerParams(vmem_limit_bytes=16 << 20),
        cost_estimate=pl.CostEstimate(
            flops=sources * rows * columns, bytes_accessed=3 << 20, transcendentals=0
        ),
        name="totals",
    )(received)


def order_kernel(runs, own_ref, other_ref, out_ref):
    rows = own_ref.shape[0] // runs
    core = lax.axis_index("K")
    for i in range(runs):
        for ref, slot in ((own_ref, core), (other_ref, 1 - core)):
            start = pl.multiple_of(slot * rows + 2 * i * rows, rows)
            out_ref[pl.ds(start, rows), :] = ref[i * rows : (i + 1) * rows, :]


def in_order(runs, own, other):
    rows, columns = own.shape
    return pl.pallas_call(
        functools.partial(order_kernel, runs),
        out_shape=jax.ShapeDtypeStruct((2 * rows, columns), BF16),
        in_specs=[VMEM] * 2,
        out_specs=VMEM,
        compiler_params=pltpu.CompilerParams(vmem_limit_bytes=4 << 20),
        cost_estimate=pl.CostEstimate(
            flops=1 << 18, bytes_accessed=1 << 19, transcendentals=0
        ),
        name="in_order",
    )(own, other)


def passed_along(value, axis, steps):
    count = lax.axis_size(axis)
    return lax.ppermute(value, axis, [(i, (i + steps) % count) for i in range(count)])


def on_device(queries, prefix_keys, cached_prefix_values, shard_len, reach, w_out):
    y_count, z_count = lax.axis_size("Y"), lax.axis_size("Z")
    shard_count = lax.axis_size(BLK)
    tokens, heads, head_size = queries.shape
    q_own = queries.reshape(tokens * heads, head_size)
    slots = prefix_keys.shape[1]
    odd = range(1, shard_count, 2)
    q_near = passed_along(q_own, BLK, 2)
    q_far = lax.ppermute(q_own, BLK, [(i, (i + 4) % shard_count) for i in odd])
    k_other = passed_along(prefix_keys[0], "K", 1)
    v_other = passed_along(cached_prefix_values[0], "K", 1)
    weights = lax.all_gather(w_out, "Y", axis=0, tiled=False)

    part_own, keys, values, meta = first_part(
        tokens, shard_len, reach, q_own, prefix_keys[0], cached_prefix_values[0]
    )
    part_far = later_part(
        third_kernel, tokens, slots, [pltpu.VMEM(q_own.shape, BF16)],
        meta, q_own, q_far, k_other, v_other,
    )
    back_far = lax.ppermute(part_far, BLK, [(i, (i - 4) % shard_count) for i in odd])
    part_near = later_part(
        second_kernel, tokens, 2 * slots, [],
        meta, q_near, keys, values, k_other, v_other,
    )
    back_near = passed_along(part_near, BLK, -2)
    spread = combine([part_own, back_near, part_far, back_far], z_count, tokens, heads)
    own = lax.all_to_all(spread, "Z", split_axis=0, concat_axis=0, tiled=True)
    other = passed_along(own, "K", 1)
    x_half = lax.axis_size("x") // 2
    pairs = []
    for y in range(lax.axis_size("y")):
        for x in range(lax.axis_size("x")):
            for big in range(y_count):
                head = (big // x_half) * 2 * x_half + (big % x_half) * 2 + x % 2
                target = head * y_count + y * x_half + x // 2
                pairs.append(((y * 2 * x_half + x) * y_count + big, target))
    placed = []
    for side in (own, other):
        partial = project(side, weights, 2)
        partial = partial.reshape(-1, *partial.shape[2:])
        received = lax.all_to_all(partial, HEADS, split_axis=0, concat_axis=0, tiled=True)
        summed = totals(received, 2)
        placed.append(lax.ppermute(summed, ("y", "x", "Y"), pairs))
    return in_order(z_count // 2, *placed)


def solution(mesh):
    finer = Mesh(mesh.devices.reshape(2, 4, 4, 8, 2), HEADS + BLK)
    placed = (
        P(BLK, HEADS, None),
        P(HEADS, BLK, None),
        P(HEADS, BLK, None),
        P(),
        P(),
        P(HEADS, BLK),
    )

    return jax.shard_map(
        on_device, mesh=finer, in_specs=placed, out_specs=P(HEADS, BLK), check_vma=False
    )
```

```python
import functools
import math

import jax
import jax.numpy as jnp
from jax import lax
from jax.experimental import pallas as pl
from jax.experimental.pallas import tpu as pltpu
from jax.sharding import Mesh
from jax.sharding import PartitionSpec as P

HEADS = ("y", "x")
BLK = ("Y", "Z", "K")
TILE = 128
NONE = -1e30
F32 = jnp.float32
BF16 = jnp.bfloat16


def eye_mask():
    rows = lax.broadcasted_iota(jnp.int32, (TILE, TILE), 0)
    lanes = lax.broadcasted_iota(jnp.int32, (TILE, TILE), 1)
    return rows == lanes


def part_body(q_ref, shards, out_ref, tokens):
    rows, head_size = q_ref.shape
    scale = head_size**-0.5 * math.log2(math.e)
    eye = eye_mask()
    stats = []
    for start in range(0, rows, TILE):
        row = start + lax.broadcasted_iota(jnp.int32, (TILE, 1), 0)
        scored = []
        for k_ref, _, length, base in shards:
            scores = lax.dot_general(
                q_ref[start : start + TILE, :],
                k_ref[...],
                (((1,), (1,)), ((), ())),
                preferred_element_type=F32,
            )
            limit = jnp.minimum(length, base + row // (rows // tokens))
            slot = lax.broadcasted_iota(jnp.int32, scores.shape, 1)
            scored.append(jnp.where(slot < limit, scores, NONE))
        top = functools.reduce(
            jnp.maximum, [jnp.max(scores, axis=1, keepdims=True) for scores in scored]
        )
        total, values = 0.0, 0.0
        for scores, (_, v_ref, _, _) in zip(scored, shards):
            weights = jnp.exp2((scores - top) * scale)
            total += jnp.sum(weights, axis=1, keepdims=True)
            values += jnp.dot(weights.astype(BF16), v_ref[...], preferred_element_type=F32)
        seen = top > 0.1 * NONE
        out_ref[start : start + TILE, :] = jnp.where(seen, values / total, 0.0).astype(BF16)
        level = jnp.where(seen, top * scale + jnp.log2(total), NONE)
        spread = jnp.where(eye, jnp.broadcast_to(level, (TILE, TILE)), 0.0)
        stats.append(jnp.sum(spread, axis=0, keepdims=True))
    level = jnp.concatenate(stats, axis=0)
    high = level.astype(BF16).astype(F32)
    middle = (level - high).astype(BF16).astype(F32)
    low = level - high - middle
    out_ref[rows:, :] = jnp.concatenate(
        [high, middle, low, jnp.zeros_like(low)], axis=0
    ).astype(BF16)


def known(meta_ref, i):
    return meta_ref[i : i + 1, 0:1]


def first_kernel(tokens, *refs):
    out_ref, k_ref, v_ref, meta_ref, lengths, reaches, q_ref, sems = refs[5:]
    copies = [
        pltpu.make_async_copy(source, target, sems.at[i])
        for i, (source, target) in enumerate(zip(refs[:5], (lengths, reaches, q_ref, k_ref, v_ref)))
    ]
    for copy in copies:
        copy.start()
    copies[0].wait()
    copies[1].wait()
    count = lengths.shape[0]
    slots = k_ref.shape[0]
    own = lax.axis_index(BLK)
    core = lax.axis_index("K")
    reach = lambda back: reaches[lax.rem(own + (count - back), count)]
    facts = (
        lengths[own],
        lengths[own + 1 - 2 * core],
        reach(0),
        reach(2) - 2 * slots,
        reach(2) - (3 - 2 * core) * slots,
        reach(4 * core) - (1 + 2 * core) * slots,
    )
    row = lax.broadcasted_iota(jnp.int32, meta_ref.shape, 0)
    meta = jnp.zeros(meta_ref.shape, jnp.int32)
    for i, fact in enumerate(facts):
        meta = jnp.where(row == i, fact, meta)
    meta_ref[...] = meta
    for copy in copies[2:]:
        copy.wait()
    part_body(q_ref, [(k_ref, v_ref, known(meta_ref, 0), known(meta_ref, 2))], out_ref, tokens)


def second_kernel(tokens, meta_ref, q_ref, k_ref, v_ref, k_other, v_other, out_ref):
    shards = [
        (k_ref, v_ref, known(meta_ref, 0), known(meta_ref, 3)),
        (k_other, v_other, known(meta_ref, 1), known(meta_ref, 4)),
    ]
    part_body(q_ref, shards, out_ref, tokens)


def third_kernel(tokens, meta_ref, q_own, q_visit, k_other, v_other, out_ref, q_ref):
    q_ref[...] = jnp.where(lax.axis_index("K") == 0, q_own[...], q_visit[...])
    shards = [(k_other, v_other, known(meta_ref, 1), known(meta_ref, 5))]
    part_body(q_ref, shards, out_ref, tokens)


def part_cost(rows, slots, head_size):
    return pl.CostEstimate(
        flops=4 * rows * slots * head_size,
        bytes_accessed=4 * slots * head_size,
        transcendentals=rows * slots,
    )


VMEM = pl.BlockSpec(memory_space=pltpu.VMEM)


def first_part(tokens, lengths, reaches, q, k, v):
    rows, head_size = q.shape
    extra = 4 * (rows // TILE)
    hbm = pl.BlockSpec(memory_space=pltpu.HBM)
    return pl.pallas_call(
        functools.partial(first_kernel, tokens),
        out_shape=(
            jax.ShapeDtypeStruct((rows + extra, head_size), BF16),
            jax.ShapeDtypeStruct(k.shape, BF16),
            jax.ShapeDtypeStruct(v.shape, BF16),
            jax.ShapeDtypeStruct((8, 128), jnp.int32),
        ),
        in_specs=[hbm] * 5,
        out_specs=(VMEM,) * 4,
        scratch_shapes=[
            pltpu.SMEM(lengths.shape, jnp.int32),
            pltpu.SMEM(reaches.shape, jnp.int32),
            pltpu.VMEM(q.shape, BF16),
            pltpu.SemaphoreType.DMA((5,)),
        ],
        compiler_params=pltpu.CompilerParams(vmem_limit_bytes=24 << 20),
        cost_estimate=part_cost(rows, k.shape[0], head_size),
        name="first_part",
    )(*(pltpu.with_memory_space_constraint(a, pltpu.HBM) for a in (lengths, reaches, q, k, v)))


def later_part(kernel, tokens, slots, scratch, *arrays):
    rows, head_size = arrays[1].shape
    extra = 4 * (rows // TILE)
    return pl.pallas_call(
        functools.partial(kernel, tokens),
        out_shape=jax.ShapeDtypeStruct((rows + extra, head_size), BF16),
        in_specs=[VMEM] * len(arrays),
        out_specs=VMEM,
        scratch_shapes=scratch,
        compiler_params=pltpu.CompilerParams(vmem_limit_bytes=24 << 20),
        cost_estimate=part_cost(rows, slots, head_size),
    )(*arrays)


def combine_kernel(*refs):
    parts, keep_ref, send_ref, total_ref = refs[:-3], refs[-3], refs[-2], refs[-1]
    head_size = parts[0].shape[1]
    groups = parts[0].shape[0] // (TILE + 4)
    rows = groups * TILE
    south = lax.axis_index("K") == 0

    def taken(part, start, stop):
        if isinstance(part, tuple):
            return jnp.where(south, part[0][start:stop, :], part[1][start:stop, :])
        return part[start:stop, :]

    parts = list(parts[:-2]) + [tuple(parts[-2:])]
    levels = []
    for part in parts:
        terms = taken(part, rows, rows + 4 * groups).astype(F32)
        levels.append(
            terms[:groups] + terms[groups : 2 * groups] + terms[2 * groups : 3 * groups]
        )
    top = functools.reduce(jnp.maximum, levels)
    factors = [jnp.exp2(level - top) for level in levels]
    inverse = 1.0 / functools.reduce(jnp.add, factors)
    eye = eye_mask()
    for group in range(groups):
        total = None
        for part, factor in zip(parts, factors):
            line = jnp.broadcast_to((factor * inverse)[group : group + 1, :], (TILE, TILE))
            column = jnp.sum(jnp.where(eye, line, 0.0), axis=1, keepdims=True)
            term = taken(part, group * TILE, (group + 1) * TILE).astype(F32) * column
            total = term if total is None else total + term
        total_ref[group * TILE : (group + 1) * TILE, :] = total
    count = keep_ref.shape[0]
    heads = rows // (2 * count)
    lead = lax.axis_index("y") == 0
    for head in range(heads):
        first = total_ref[pl.ds(head, count, stride=heads), :].astype(BF16)
        second = total_ref[pl.ds(heads * count + head, count, stride=heads), :].astype(BF16)
        columns = slice(head * head_size, (head + 1) * head_size)
        keep_ref[:, columns] = jnp.where(lead, first, second)
        send_ref[:, columns] = jnp.where(lead, second, first)


def combine(parts, tokens, heads):
    head_size = parts[0].shape[1]
    half = jax.ShapeDtypeStruct((tokens // 2, heads * head_size), BF16)
    return pl.pallas_call(
        combine_kernel,
        out_shape=(half, half),
        in_specs=[VMEM] * len(parts),
        out_specs=(VMEM, VMEM),
        scratch_shapes=[pltpu.VMEM((heads * tokens, head_size), F32)],
        compiler_params=pltpu.CompilerParams(vmem_limit_bytes=8 << 20),
        cost_estimate=pl.CostEstimate(
            flops=1 << 20, bytes_accessed=1 << 20, transcendentals=0
        ),
        name="combine",
    )(*parts)


def widen_kernel(keep_ref, got_ref, out_ref):
    width = keep_ref.shape[1]
    for copy in range(out_ref.shape[0]):
        out_ref[copy, :, :width] = keep_ref[...]
        out_ref[copy, :, width:] = got_ref[...]


def widen(keep, got, copies):
    rows, width = keep.shape
    return pl.pallas_call(
        widen_kernel,
        out_shape=jax.ShapeDtypeStruct((copies, rows, 2 * width), BF16),
        in_specs=[VMEM] * 2,
        out_specs=VMEM,
        compiler_params=pltpu.CompilerParams(vmem_limit_bytes=8 << 20),
        cost_estimate=pl.CostEstimate(
            flops=1 << 18, bytes_accessed=1 << 20, transcendentals=0
        ),
        name="widen",
    )(keep, got)


def project_kernel(own_ref, other_ref, w_ref, out_ref):
    groups, rows, width = own_ref.shape
    depth = width // 2
    pair = lax.axis_index("y")
    w_own, w_other = w_ref[pair], w_ref[1 - pair]
    for slot, ref in enumerate((own_ref, other_ref)):
        lhs = ref[...].reshape(groups * rows, width)
        part = jnp.dot(lhs[:, :depth], w_own, preferred_element_type=F32)
        part += jnp.dot(lhs[:, depth:], w_other, preferred_element_type=F32)
        part = part.astype(BF16)
        half = groups * rows // 2
        for i in range(2):
            out_ref[0, i, 0, slot * half : (slot + 1) * half, :] = part[i * half : (i + 1) * half]


def project(own, other, weights):
    groups, rows, width = own.shape
    depth, columns = weights.shape[1:]
    pieces = weights.shape[0] // 2
    side = pl.BlockSpec((groups, rows, width), lambda i: (0, 0, 0))
    return pl.pallas_call(
        project_kernel,
        grid=(pieces,),
        out_shape=pltpu.HBM((pieces // 2, 2, 2, groups * rows, columns), BF16),
        in_specs=[side, side, pl.BlockSpec((2, depth, columns), lambda i: (i, 0, 0))],
        out_specs=pl.BlockSpec(
            (1, 2, 1, groups * rows, columns), lambda i: (i // 2, 0, i % 2, 0, 0)
        ),
        compiler_params=pltpu.CompilerParams(vmem_limit_bytes=24 << 20),
        cost_estimate=pl.CostEstimate(
            flops=4 * groups * rows * width * columns * pieces,
            bytes_accessed=6 << 20,
            transcendentals=0,
        ),
        name="project",
    )(own, other, pltpu.with_memory_space_constraint(weights, pltpu.HBM))


def total_kernel(in_ref, *out_refs):
    rows = in_ref.shape[2]
    step = 64
    for k, out_ref in enumerate(out_refs):
        piece = lax.rem(lax.axis_index("y") + k, 2)
        for start in range(0, rows, step):
            total = in_ref[0, piece, start : start + step, :].astype(F32)
            for i in range(1, in_ref.shape[0]):
                total += in_ref[i, piece, start : start + step, :].astype(F32)
            out_ref[start : start + step, :] = total.astype(BF16)


def totals(received):
    sources, count, rows, columns = received.shape
    return pl.pallas_call(
        total_kernel,
        out_shape=[jax.ShapeDtypeStruct((rows, columns), BF16)] * count,
        in_specs=[VMEM],
        out_specs=[VMEM] * count,
        compiler_params=pltpu.CompilerParams(vmem_limit_bytes=16 << 20),
        cost_estimate=pl.CostEstimate(
            flops=sources * count * rows * columns, bytes_accessed=2 << 20, transcendentals=0
        ),
        name="totals",
    )(received)


def order_kernel(runs, *refs):
    pieces, out_ref = refs[:-1], refs[-1]
    rows = pieces[0].shape[0] // (2 * runs)
    core, big = lax.axis_index("K"), lax.axis_index("Y")
    for k, ref in enumerate(pieces):
        half = lax.rem(big + k, 2)
        for slot, held in enumerate((core, 1 - core)):
            for i in range(runs):
                start = pl.multiple_of(((2 * i + held) * 2 + half) * rows, rows)
                source = (slot * runs + i) * rows
                out_ref[pl.ds(start, rows), :] = ref[source : source + rows, :]


def in_order(runs, pieces):
    rows, columns = pieces[0].shape
    return pl.pallas_call(
        functools.partial(order_kernel, runs),
        out_shape=jax.ShapeDtypeStruct((2 * rows, columns), BF16),
        in_specs=[VMEM] * 2,
        out_specs=VMEM,
        compiler_params=pltpu.CompilerParams(vmem_limit_bytes=4 << 20),
        cost_estimate=pl.CostEstimate(
            flops=1 << 18, bytes_accessed=1 << 19, transcendentals=0
        ),
        name="in_order",
    )(*pieces)


def passed_along(value, axis, steps):
    count = lax.axis_size(axis)
    return lax.ppermute(value, axis, [(i, (i + steps) % count) for i in range(count)])


def on_device(queries, prefix_keys, cached_prefix_values, shard_len, reach, w_out):
    y_count, z_count = lax.axis_size("Y"), lax.axis_size("Z")
    shard_count = lax.axis_size(BLK)
    tokens, heads, head_size = queries.shape
    q_own = queries.reshape(tokens * heads, head_size)
    slots = prefix_keys.shape[1]
    odd = range(1, shard_count, 2)
    q_near = passed_along(q_own, BLK, 2)
    q_far = lax.ppermute(q_own, BLK, [(i, (i + 4) % shard_count) for i in odd])
    k_other = passed_along(prefix_keys[0], "K", 1)
    v_other = passed_along(cached_prefix_values[0], "K", 1)
    weights = lax.all_gather(w_out, ("Y", "y"), axis=0, tiled=False)

    part_own, keys, values, meta = first_part(
        tokens, shard_len, reach, q_own, prefix_keys[0], cached_prefix_values[0]
    )
    part_near = later_part(
        second_kernel, tokens, 2 * slots, [],
        meta, q_near, keys, values, k_other, v_other,
    )
    back_near = passed_along(part_near, BLK, -2)
    part_far = later_part(
        third_kernel, tokens, slots, [pltpu.VMEM(q_own.shape, BF16)],
        meta, q_own, q_far, k_other, v_other,
    )
    back_far = lax.ppermute(part_far, BLK, [(i, (i - 4) % shard_count) for i in odd])
    keep, send = combine([part_own, back_near, part_far, back_far], tokens, heads)
    got = passed_along(send, "y", 1)
    wide = widen(keep, got, z_count)
    own = lax.all_to_all(wide, "Z", split_axis=0, concat_axis=0, tiled=True)
    other = passed_along(own, "K", 1)
    partial = project(own, other, weights)
    partial = partial.reshape(-1, *partial.shape[2:])
    received = lax.all_to_all(partial, "x", split_axis=0, concat_axis=0, tiled=True)
    summed = totals(received)
    placed = []
    for k in range(2):
        pairs = []
        for y in range(2):
            for x in range(lax.axis_size("x")):
                for big in range(y_count):
                    head = (big // 2) * 4 + (big % 2) * 2 + x % 2
                    target = head * y_count + (x // 2) * 2 + (y + k) % 2
                    pairs.append(((y * 4 + x) * y_count + big, target))
        placed.append(lax.ppermute(summed[k], ("y", "x", "Y"), pairs))
    return in_order(z_count // 2, placed)


def solution(mesh):
    finer = Mesh(mesh.devices.reshape(2, 4, 4, 8, 2), HEADS + BLK)
    placed = (
        P(BLK, HEADS, None),
        P(HEADS, BLK, None),
        P(HEADS, BLK, None),
        P(),
        P(),
        P(HEADS, BLK),
    )

    return jax.shard_map(
        on_device, mesh=finer, in_specs=placed, out_specs=P(HEADS, BLK), check_vma=False
    )
```

```python
import functools
import math

import jax
import jax.numpy as jnp
from jax import lax
from jax.experimental import pallas as pl
from jax.experimental.pallas import tpu as pltpu
from jax.sharding import Mesh
from jax.sharding import PartitionSpec as P

HEADS = ("y", "x")
BLK = ("Y", "Z", "K")
TILE = 128
NONE = -1e30
F32 = jnp.float32
BF16 = jnp.bfloat16


def eye_mask():
    rows = lax.broadcasted_iota(jnp.int32, (TILE, TILE), 0)
    lanes = lax.broadcasted_iota(jnp.int32, (TILE, TILE), 1)
    return rows == lanes


def part_body(q_ref, shards, out_ref, tokens):
    rows, head_size = q_ref.shape
    scale = head_size**-0.5 * math.log2(math.e)
    eye = eye_mask()
    stats = []
    for start in range(0, rows, TILE):
        row = start + lax.broadcasted_iota(jnp.int32, (TILE, 1), 0)
        scored = []
        for k_ref, _, length, base in shards:
            scores = lax.dot_general(
                q_ref[start : start + TILE, :],
                k_ref[...],
                (((1,), (1,)), ((), ())),
                preferred_element_type=F32,
            )
            limit = jnp.minimum(length, base + row // (rows // tokens))
            slot = lax.broadcasted_iota(jnp.int32, scores.shape, 1)
            scored.append(jnp.where(slot < limit, scores, NONE))
        top = functools.reduce(
            jnp.maximum, [jnp.max(scores, axis=1, keepdims=True) for scores in scored]
        )
        total, values = 0.0, 0.0
        for scores, (_, v_ref, _, _) in zip(scored, shards):
            weights = jnp.exp2((scores - top) * scale)
            total += jnp.sum(weights, axis=1, keepdims=True)
            values += jnp.dot(weights.astype(BF16), v_ref[...], preferred_element_type=F32)
        seen = top > 0.1 * NONE
        out_ref[start : start + TILE, :] = jnp.where(seen, values / total, 0.0).astype(BF16)
        level = jnp.where(seen, top * scale + jnp.log2(total), NONE)
        spread = jnp.where(eye, jnp.broadcast_to(level, (TILE, TILE)), 0.0)
        stats.append(jnp.sum(spread, axis=0, keepdims=True))
    level = jnp.concatenate(stats, axis=0)
    high = level.astype(BF16).astype(F32)
    middle = (level - high).astype(BF16).astype(F32)
    low = level - high - middle
    out_ref[rows:, :] = jnp.concatenate(
        [high, middle, low, jnp.zeros_like(low)], axis=0
    ).astype(BF16)


def known(meta_ref, i):
    return meta_ref[i : i + 1, 0:1]


def first_kernel(tokens, *refs):
    out_ref, k_ref, v_ref, meta_ref, lengths, reaches, q_ref, sems = refs[5:]
    copies = [
        pltpu.make_async_copy(source, target, sems.at[i])
        for i, (source, target) in enumerate(zip(refs[:5], (lengths, reaches, q_ref, k_ref, v_ref)))
    ]
    for copy in copies:
        copy.start()
    copies[0].wait()
    copies[1].wait()
    count = lengths.shape[0]
    slots = k_ref.shape[0]
    own = lax.axis_index(BLK)
    core = lax.axis_index("K")
    reach = lambda back: reaches[lax.rem(own + (count - back), count)]
    facts = (
        lengths[own],
        lengths[own + 1 - 2 * core],
        reach(0),
        reach(2) - 2 * slots,
        reach(2) - (3 - 2 * core) * slots,
        reach(4 * core) - (1 + 2 * core) * slots,
    )
    row = lax.broadcasted_iota(jnp.int32, meta_ref.shape, 0)
    meta = jnp.zeros(meta_ref.shape, jnp.int32)
    for i, fact in enumerate(facts):
        meta = jnp.where(row == i, fact, meta)
    meta_ref[...] = meta
    for copy in copies[2:]:
        copy.wait()
    part_body(q_ref, [(k_ref, v_ref, known(meta_ref, 0), known(meta_ref, 2))], out_ref, tokens)


def second_kernel(tokens, meta_ref, q_ref, k_ref, v_ref, k_other, v_other, out_ref):
    shards = [
        (k_ref, v_ref, known(meta_ref, 0), known(meta_ref, 3)),
        (k_other, v_other, known(meta_ref, 1), known(meta_ref, 4)),
    ]
    part_body(q_ref, shards, out_ref, tokens)


def third_kernel(tokens, meta_ref, q_own, q_visit, k_other, v_other, out_ref, q_ref):
    q_ref[...] = jnp.where(lax.axis_index("K") == 0, q_own[...], q_visit[...])
    shards = [(k_other, v_other, known(meta_ref, 1), known(meta_ref, 5))]
    part_body(q_ref, shards, out_ref, tokens)


def part_cost(rows, slots, head_size):
    return pl.CostEstimate(
        flops=4 * rows * slots * head_size,
        bytes_accessed=4 * slots * head_size,
        transcendentals=rows * slots,
    )


VMEM = pl.BlockSpec(memory_space=pltpu.VMEM)


def first_part(tokens, lengths, reaches, q, k, v):
    rows, head_size = q.shape
    extra = 4 * (rows // TILE)
    hbm = pl.BlockSpec(memory_space=pltpu.HBM)
    return pl.pallas_call(
        functools.partial(first_kernel, tokens),
        out_shape=(
            jax.ShapeDtypeStruct((rows + extra, head_size), BF16),
            jax.ShapeDtypeStruct(k.shape, BF16),
            jax.ShapeDtypeStruct(v.shape, BF16),
            jax.ShapeDtypeStruct((8, 128), jnp.int32),
        ),
        in_specs=[hbm] * 5,
        out_specs=(VMEM,) * 4,
        scratch_shapes=[
            pltpu.SMEM(lengths.shape, jnp.int32),
            pltpu.SMEM(reaches.shape, jnp.int32),
            pltpu.VMEM(q.shape, BF16),
            pltpu.SemaphoreType.DMA((5,)),
        ],
        compiler_params=pltpu.CompilerParams(vmem_limit_bytes=24 << 20),
        cost_estimate=part_cost(rows, k.shape[0], head_size),
        name="first_part",
    )(*(pltpu.with_memory_space_constraint(a, pltpu.HBM) for a in (lengths, reaches, q, k, v)))


def later_part(kernel, tokens, slots, scratch, *arrays):
    rows, head_size = arrays[1].shape
    extra = 4 * (rows // TILE)
    return pl.pallas_call(
        functools.partial(kernel, tokens),
        out_shape=jax.ShapeDtypeStruct((rows + extra, head_size), BF16),
        in_specs=[VMEM] * len(arrays),
        out_specs=VMEM,
        scratch_shapes=scratch,
        compiler_params=pltpu.CompilerParams(vmem_limit_bytes=24 << 20),
        cost_estimate=part_cost(rows, slots, head_size),
    )(*arrays)


def combine_kernel(*refs):
    parts, out_ref, total_ref = refs[:-2], refs[-2], refs[-1]
    head_size = parts[0].shape[1]
    groups = parts[0].shape[0] // (TILE + 4)
    rows = groups * TILE
    south = lax.axis_index("K") == 0

    def taken(part, start, stop):
        if isinstance(part, tuple):
            return jnp.where(south, part[0][start:stop, :], part[1][start:stop, :])
        return part[start:stop, :]

    parts = list(parts[:-2]) + [tuple(parts[-2:])]
    levels = []
    for part in parts:
        terms = taken(part, rows, rows + 4 * groups).astype(F32)
        levels.append(
            terms[:groups] + terms[groups : 2 * groups] + terms[2 * groups : 3 * groups]
        )
    top = functools.reduce(jnp.maximum, levels)
    factors = [jnp.exp2(level - top) for level in levels]
    inverse = 1.0 / functools.reduce(jnp.add, factors)
    eye = eye_mask()
    for group in range(groups):
        total = None
        for part, factor in zip(parts, factors):
            line = jnp.broadcast_to((factor * inverse)[group : group + 1, :], (TILE, TILE))
            column = jnp.sum(jnp.where(eye, line, 0.0), axis=1, keepdims=True)
            term = taken(part, group * TILE, (group + 1) * TILE).astype(F32) * column
            total = term if total is None else total + term
        total_ref[group * TILE : (group + 1) * TILE, :] = total
    copies, count, _ = out_ref.shape
    heads = rows // (2 * count)
    for head in range(heads):
        columns = slice(head * head_size, (head + 1) * head_size)
        for half in range(2):
            start = half * heads * count + head
            piece = total_ref[pl.ds(start, count, stride=heads), :].astype(BF16)
            for copy in range(half * copies // 2, (half + 1) * copies // 2):
                out_ref[copy, :, columns] = piece


def combine(parts, copies, tokens, heads):
    head_size = parts[0].shape[1]
    return pl.pallas_call(
        combine_kernel,
        out_shape=jax.ShapeDtypeStruct((2 * copies, tokens // 2, heads * head_size), BF16),
        in_specs=[VMEM] * len(parts),
        out_specs=VMEM,
        scratch_shapes=[pltpu.VMEM((heads * tokens, head_size), F32)],
        compiler_params=pltpu.CompilerParams(vmem_limit_bytes=8 << 20),
        cost_estimate=pl.CostEstimate(
            flops=1 << 20, bytes_accessed=1 << 20, transcendentals=0
        ),
        name="combine",
    )(*parts)


def project_kernel(own_ref, other_ref, w_ref, out_ref):
    groups, rows, depth = own_ref.shape
    count = groups // 2
    half = count * rows // 2
    for slot, ref in enumerate((own_ref, other_ref)):
        part = None
        for i in range(2):
            lhs = ref[i * count : (i + 1) * count].reshape(count * rows, depth)
            term = jnp.dot(lhs, w_ref[i], preferred_element_type=F32)
            part = term if part is None else part + term
        part = part.astype(BF16)
        for i in range(2):
            out_ref[0, i, 0, slot * half : (slot + 1) * half, :] = part[i * half : (i + 1) * half]


def project(own, other, weights):
    groups, rows, depth = own.shape
    columns = weights.shape[2]
    pieces = weights.shape[0] // 2
    held = groups * rows
    side = pl.BlockSpec((groups, rows, depth), lambda i: (0, 0, 0))
    return pl.pallas_call(
        project_kernel,
        grid=(pieces,),
        out_shape=pltpu.HBM((pieces // 2, 2, 2, held // 2, columns), BF16),
        in_specs=[side, side, pl.BlockSpec((2, depth, columns), lambda i: (i, 0, 0))],
        out_specs=pl.BlockSpec(
            (1, 2, 1, held // 2, columns), lambda i: (i // 2, 0, i % 2, 0, 0)
        ),
        compiler_params=pltpu.CompilerParams(vmem_limit_bytes=24 << 20),
        cost_estimate=pl.CostEstimate(
            flops=4 * held * depth * columns * pieces,
            bytes_accessed=6 << 20,
            transcendentals=0,
        ),
        name="project",
    )(own, other, pltpu.with_memory_space_constraint(weights, pltpu.HBM))


def total_kernel(in_ref, *out_refs):
    rows = in_ref.shape[2]
    step = 64
    for k, out_ref in enumerate(out_refs):
        piece = lax.rem(lax.axis_index("y") + k, 2)
        for start in range(0, rows, step):
            total = in_ref[0, piece, start : start + step, :].astype(F32)
            for i in range(1, in_ref.shape[0]):
                total += in_ref[i, piece, start : start + step, :].astype(F32)
            out_ref[start : start + step, :] = total.astype(BF16)


def totals(received):
    sources, count, rows, columns = received.shape
    return pl.pallas_call(
        total_kernel,
        out_shape=[jax.ShapeDtypeStruct((rows, columns), BF16)] * count,
        in_specs=[VMEM],
        out_specs=[VMEM] * count,
        compiler_params=pltpu.CompilerParams(vmem_limit_bytes=16 << 20),
        cost_estimate=pl.CostEstimate(
            flops=sources * count * rows * columns, bytes_accessed=2 << 20, transcendentals=0
        ),
        name="totals",
    )(received)


def order_kernel(runs, *refs):
    pieces, out_ref = refs[:-1], refs[-1]
    rows = pieces[0].shape[0] // (2 * runs)
    core, big = lax.axis_index("K"), lax.axis_index("Y")
    for k, ref in enumerate(pieces):
        half = lax.rem(big + k, 2)
        for slot, held in enumerate((core, 1 - core)):
            for i in range(runs):
                start = pl.multiple_of(((2 * i + held) * 2 + half) * rows, rows)
                source = (slot * runs + i) * rows
                out_ref[pl.ds(start, rows), :] = ref[source : source + rows, :]


def in_order(runs, pieces):
    rows, columns = pieces[0].shape
    return pl.pallas_call(
        functools.partial(order_kernel, runs),
        out_shape=jax.ShapeDtypeStruct((2 * rows, columns), BF16),
        in_specs=[VMEM] * 2,
        out_specs=VMEM,
        compiler_params=pltpu.CompilerParams(vmem_limit_bytes=4 << 20),
        cost_estimate=pl.CostEstimate(
            flops=1 << 18, bytes_accessed=1 << 19, transcendentals=0
        ),
        name="in_order",
    )(*pieces)


def passed_along(value, axis, steps):
    count = lax.axis_size(axis)
    return lax.ppermute(value, axis, [(i, (i + steps) % count) for i in range(count)])


def on_device(queries, prefix_keys, cached_prefix_values, shard_len, reach, w_out):
    y_count, z_count = lax.axis_size("Y"), lax.axis_size("Z")
    shard_count = lax.axis_size(BLK)
    tokens, heads, head_size = queries.shape
    q_own = queries.reshape(tokens * heads, head_size)
    slots = prefix_keys.shape[1]
    odd = range(1, shard_count, 2)
    q_near = passed_along(q_own, BLK, 2)
    q_far = lax.ppermute(q_own, BLK, [(i, (i + 4) % shard_count) for i in odd])
    k_other = passed_along(prefix_keys[0], "K", 1)
    v_other = passed_along(cached_prefix_values[0], "K", 1)
    weights = lax.all_gather(w_out, ("Y", "y"), axis=0, tiled=False)

    part_own, keys, values, meta = first_part(
        tokens, shard_len, reach, q_own, prefix_keys[0], cached_prefix_values[0]
    )
    part_near = later_part(
        second_kernel, tokens, 2 * slots, [],
        meta, q_near, keys, values, k_other, v_other,
    )
    back_near = passed_along(part_near, BLK, -2)
    part_far = later_part(
        third_kernel, tokens, slots, [pltpu.VMEM(q_own.shape, BF16)],
        meta, q_own, q_far, k_other, v_other,
    )
    back_far = lax.ppermute(part_far, BLK, [(i, (i - 4) % shard_count) for i in odd])
    halves = combine([part_own, back_near, part_far, back_far], z_count, tokens, heads)
    own = lax.all_to_all(halves, ("y", "Z"), split_axis=0, concat_axis=0, tiled=True)
    other = passed_along(own, "K", 1)
    partial = project(own, other, weights)
    partial = partial.reshape(-1, *partial.shape[2:])
    received = lax.all_to_all(partial, "x", split_axis=0, concat_axis=0, tiled=True)
    summed = totals(received)
    placed = []
    for k in range(2):
        pairs = []
        for y in range(2):
            for x in range(lax.axis_size("x")):
                for big in range(y_count):
                    head = (big // 2) * 4 + (big % 2) * 2 + x % 2
                    target = head * y_count + (x // 2) * 2 + (y + k) % 2
                    pairs.append(((y * 4 + x) * y_count + big, target))
        placed.append(lax.ppermute(summed[k], ("y", "x", "Y"), pairs))
    return in_order(z_count // 2, placed)


def solution(mesh):
    finer = Mesh(mesh.devices.reshape(2, 4, 4, 8, 2), HEADS + BLK)
    placed = (
        P(BLK, HEADS, None),
        P(HEADS, BLK, None),
        P(HEADS, BLK, None),
        P(),
        P(),
        P(HEADS, BLK),
    )

    return jax.shard_map(
        on_device, mesh=finer, in_specs=placed, out_specs=P(HEADS, BLK), check_vma=False
    )
```

```python
import functools
import math

import jax
import jax.numpy as jnp
from jax import lax
from jax.experimental import pallas as pl
from jax.experimental.pallas import tpu as pltpu
from jax.sharding import Mesh
from jax.sharding import PartitionSpec as P

HEADS = ("y", "x")
BLK = ("Y", "Z", "K")
TILE = 128
NONE = -1e30
F32 = jnp.float32
BF16 = jnp.bfloat16


def eye_mask():
    rows = lax.broadcasted_iota(jnp.int32, (TILE, TILE), 0)
    lanes = lax.broadcasted_iota(jnp.int32, (TILE, TILE), 1)
    return rows == lanes


def part_body(q_ref, shards, out_ref, tokens):
    rows, head_size = q_ref.shape
    scale = head_size**-0.5 * math.log2(math.e)
    eye = eye_mask()
    stats = []
    for start in range(0, rows, TILE):
        row = start + lax.broadcasted_iota(jnp.int32, (TILE, 1), 0)
        scored = []
        for k_ref, _, length, base in shards:
            scores = lax.dot_general(
                q_ref[start : start + TILE, :],
                k_ref[...],
                (((1,), (1,)), ((), ())),
                preferred_element_type=F32,
            )
            limit = jnp.minimum(length, base + row // (rows // tokens))
            slot = lax.broadcasted_iota(jnp.int32, scores.shape, 1)
            scored.append(jnp.where(slot < limit, scores, NONE))
        top = functools.reduce(
            jnp.maximum, [jnp.max(scores, axis=1, keepdims=True) for scores in scored]
        )
        total, values = 0.0, 0.0
        for scores, (_, v_ref, _, _) in zip(scored, shards):
            weights = jnp.exp2((scores - top) * scale)
            total += jnp.sum(weights, axis=1, keepdims=True)
            values += jnp.dot(weights.astype(BF16), v_ref[...], preferred_element_type=F32)
        seen = top > 0.1 * NONE
        out_ref[start : start + TILE, :] = jnp.where(seen, values / total, 0.0).astype(BF16)
        level = jnp.where(seen, top * scale + jnp.log2(total), NONE)
        spread = jnp.where(eye, jnp.broadcast_to(level, (TILE, TILE)), 0.0)
        stats.append(jnp.sum(spread, axis=0, keepdims=True))
    level = jnp.concatenate(stats, axis=0)
    high = level.astype(BF16).astype(F32)
    middle = (level - high).astype(BF16).astype(F32)
    low = level - high - middle
    out_ref[rows:, :] = jnp.concatenate(
        [high, middle, low, jnp.zeros_like(low)], axis=0
    ).astype(BF16)


def known(meta_ref, i):
    return meta_ref[i : i + 1, 0:1]


def first_kernel(tokens, *refs):
    out_ref, k_ref, v_ref, meta_ref, lengths, reaches, q_ref, sems = refs[5:]
    copies = [
        pltpu.make_async_copy(source, target, sems.at[i])
        for i, (source, target) in enumerate(zip(refs[:5], (lengths, reaches, q_ref, k_ref, v_ref)))
    ]
    for copy in copies:
        copy.start()
    copies[0].wait()
    copies[1].wait()
    count = lengths.shape[0]
    slots = k_ref.shape[0]
    own = lax.axis_index(BLK)
    core = lax.axis_index("K")
    reach = lambda back: reaches[lax.rem(own + (count - back), count)]
    facts = (
        lengths[own],
        lengths[own + 1 - 2 * core],
        reach(0),
        reach(2) - 2 * slots,
        reach(2) - (3 - 2 * core) * slots,
        reach(4 * core) - (1 + 2 * core) * slots,
    )
    row = lax.broadcasted_iota(jnp.int32, meta_ref.shape, 0)
    meta = jnp.zeros(meta_ref.shape, jnp.int32)
    for i, fact in enumerate(facts):
        meta = jnp.where(row == i, fact, meta)
    meta_ref[...] = meta
    for copy in copies[2:]:
        copy.wait()
    part_body(q_ref, [(k_ref, v_ref, known(meta_ref, 0), known(meta_ref, 2))], out_ref, tokens)


def second_kernel(tokens, meta_ref, q_ref, k_ref, v_ref, k_other, v_other, out_ref):
    shards = [
        (k_ref, v_ref, known(meta_ref, 0), known(meta_ref, 3)),
        (k_other, v_other, known(meta_ref, 1), known(meta_ref, 4)),
    ]
    part_body(q_ref, shards, out_ref, tokens)


def third_kernel(tokens, meta_ref, q_own, q_visit, k_other, v_other, out_ref, q_ref):
    q_ref[...] = jnp.where(lax.axis_index("K") == 0, q_own[...], q_visit[...])
    shards = [(k_other, v_other, known(meta_ref, 1), known(meta_ref, 5))]
    part_body(q_ref, shards, out_ref, tokens)


def part_cost(rows, slots, head_size):
    return pl.CostEstimate(
        flops=4 * rows * slots * head_size,
        bytes_accessed=4 * slots * head_size,
        transcendentals=rows * slots,
    )


VMEM = pl.BlockSpec(memory_space=pltpu.VMEM)


def first_part(tokens, lengths, reaches, q, k, v):
    rows, head_size = q.shape
    extra = 4 * (rows // TILE)
    hbm = pl.BlockSpec(memory_space=pltpu.HBM)
    return pl.pallas_call(
        functools.partial(first_kernel, tokens),
        out_shape=(
            jax.ShapeDtypeStruct((rows + extra, head_size), BF16),
            jax.ShapeDtypeStruct(k.shape, BF16),
            jax.ShapeDtypeStruct(v.shape, BF16),
            jax.ShapeDtypeStruct((8, 128), jnp.int32),
        ),
        in_specs=[hbm] * 5,
        out_specs=(VMEM,) * 4,
        scratch_shapes=[
            pltpu.SMEM(lengths.shape, jnp.int32),
            pltpu.SMEM(reaches.shape, jnp.int32),
            pltpu.VMEM(q.shape, BF16),
            pltpu.SemaphoreType.DMA((5,)),
        ],
        compiler_params=pltpu.CompilerParams(vmem_limit_bytes=24 << 20),
        cost_estimate=part_cost(rows, k.shape[0], head_size),
        name="first_part",
    )(*(pltpu.with_memory_space_constraint(a, pltpu.HBM) for a in (lengths, reaches, q, k, v)))


def later_part(kernel, tokens, slots, scratch, *arrays):
    rows, head_size = arrays[1].shape
    extra = 4 * (rows // TILE)
    return pl.pallas_call(
        functools.partial(kernel, tokens),
        out_shape=jax.ShapeDtypeStruct((rows + extra, head_size), BF16),
        in_specs=[VMEM] * len(arrays),
        out_specs=VMEM,
        scratch_shapes=scratch,
        compiler_params=pltpu.CompilerParams(vmem_limit_bytes=24 << 20),
        cost_estimate=part_cost(rows, slots, head_size),
    )(*arrays)


def combine_kernel(*refs):
    parts, out_ref, total_ref = refs[:-2], refs[-2], refs[-1]
    head_size = parts[0].shape[1]
    groups = parts[0].shape[0] // (TILE + 4)
    rows = groups * TILE
    south = lax.axis_index("K") == 0

    def taken(part, start, stop):
        if isinstance(part, tuple):
            return jnp.where(south, part[0][start:stop, :], part[1][start:stop, :])
        return part[start:stop, :]

    parts = list(parts[:-2]) + [tuple(parts[-2:])]
    levels = []
    for part in parts:
        terms = taken(part, rows, rows + 4 * groups).astype(F32)
        levels.append(
            terms[:groups] + terms[groups : 2 * groups] + terms[2 * groups : 3 * groups]
        )
    top = functools.reduce(jnp.maximum, levels)
    factors = [jnp.exp2(level - top) for level in levels]
    inverse = 1.0 / functools.reduce(jnp.add, factors)
    eye = eye_mask()
    for group in range(groups):
        total = None
        for part, factor in zip(parts, factors):
            line = jnp.broadcast_to((factor * inverse)[group : group + 1, :], (TILE, TILE))
            column = jnp.sum(jnp.where(eye, line, 0.0), axis=1, keepdims=True)
            term = taken(part, group * TILE, (group + 1) * TILE).astype(F32) * column
            total = term if total is None else total + term
        total_ref[group * TILE : (group + 1) * TILE, :] = total
    copies, count, _ = out_ref.shape
    heads = rows // (2 * count)
    for head in range(heads):
        columns = slice(head * head_size, (head + 1) * head_size)
        for half in range(2):
            start = half * heads * count + head
            piece = total_ref[pl.ds(start, count, stride=heads), :].astype(BF16)
            for copy in range(half * copies // 2, (half + 1) * copies // 2):
                out_ref[copy, :, columns] = piece


def combine(parts, copies, tokens, heads):
    head_size = parts[0].shape[1]
    return pl.pallas_call(
        combine_kernel,
        out_shape=jax.ShapeDtypeStruct((2 * copies, tokens // 2, heads * head_size), BF16),
        in_specs=[VMEM] * len(parts),
        out_specs=VMEM,
        scratch_shapes=[pltpu.VMEM((heads * tokens, head_size), F32)],
        compiler_params=pltpu.CompilerParams(vmem_limit_bytes=8 << 20),
        cost_estimate=pl.CostEstimate(
            flops=1 << 20, bytes_accessed=1 << 20, transcendentals=0
        ),
        name="combine",
    )(*parts)


def project_kernel(own_ref, other_ref, w_ref, out_ref):
    groups, rows, depth = own_ref.shape
    count = groups // 2
    part = None
    for i in range(2):
        sides = [ref[i * count : (i + 1) * count] for ref in (own_ref, other_ref)]
        lhs = jnp.concatenate([side.reshape(count * rows, depth) for side in sides], axis=0)
        term = jnp.dot(lhs, w_ref[i], preferred_element_type=F32)
        part = term if part is None else part + term
    part = part.astype(BF16)
    half = count * rows // 2
    for slot in range(2):
        for i in range(2):
            start = (2 * slot + i) * half
            out_ref[0, i, slot * half : (slot + 1) * half, :] = part[start : start + half]


def project(own, other, weights):
    groups, rows, depth = own.shape
    columns = weights.shape[2]
    pieces = weights.shape[0] // 2
    held = groups * rows
    side = pl.BlockSpec((groups, rows, depth), lambda i: (0, 0, 0))
    return pl.pallas_call(
        project_kernel,
        grid=(pieces,),
        out_shape=pltpu.HBM((pieces, 2, held // 2, columns), BF16),
        in_specs=[side, side, pl.BlockSpec((2, depth, columns), lambda i: (i, 0, 0))],
        out_specs=pl.BlockSpec((1, 2, held // 2, columns), lambda i: (i, 0, 0, 0)),
        compiler_params=pltpu.CompilerParams(vmem_limit_bytes=24 << 20),
        cost_estimate=pl.CostEstimate(
            flops=4 * held * depth * columns * pieces,
            bytes_accessed=6 << 20,
            transcendentals=0,
        ),
        name="project",
    )(own, other, pltpu.with_memory_space_constraint(weights, pltpu.HBM))


def total_kernel(runs, in_ref, out_ref):
    sources = in_ref.shape[0] // 2
    rows = in_ref.shape[1] // (2 * runs)
    core = lax.axis_index("K")
    for half in range(2):
        for slot, held in enumerate((core, 1 - core)):
            for i in range(runs):
                lines = slice((slot * runs + i) * rows, (slot * runs + i + 1) * rows)
                total = in_ref[half * sources, lines, :].astype(F32)
                for source in range(half * sources + 1, (half + 1) * sources):
                    total += in_ref[source, lines, :].astype(F32)
                start = pl.multiple_of(((2 * i + held) * 2 + half) * rows, rows)
                out_ref[pl.ds(start, rows), :] = total.astype(BF16)


def totals(received, runs):
    sources, rows, columns = received.shape
    return pl.pallas_call(
        functools.partial(total_kernel, runs),
        out_shape=jax.ShapeDtypeStruct((2 * rows, columns), BF16),
        in_specs=[VMEM],
        out_specs=VMEM,
        compiler_params=pltpu.CompilerParams(vmem_limit_bytes=16 << 20),
        cost_estimate=pl.CostEstimate(
            flops=sources * rows * columns, bytes_accessed=2 << 20, transcendentals=0
        ),
        name="totals",
    )(received)


def passed_along(value, axis, steps):
    count = lax.axis_size(axis)
    return lax.ppermute(value, axis, [(i, (i + steps) % count) for i in range(count)])


def on_device(queries, prefix_keys, cached_prefix_values, shard_len, reach, w_out):
    y_count, z_count = lax.axis_size("Y"), lax.axis_size("Z")
    shard_count = lax.axis_size(BLK)
    tokens, heads, head_size = queries.shape
    q_own = queries.reshape(tokens * heads, head_size)
    slots = prefix_keys.shape[1]
    odd = range(1, shard_count, 2)
    q_near = passed_along(q_own, BLK, 2)
    q_far = lax.ppermute(q_own, BLK, [(i, (i + 4) % shard_count) for i in odd])
    k_other = passed_along(prefix_keys[0], "K", 1)
    v_other = passed_along(cached_prefix_values[0], "K", 1)
    weights = lax.all_gather(w_out, ("Y", "y"), axis=0, tiled=False)

    part_own, keys, values, meta = first_part(
        tokens, shard_len, reach, q_own, prefix_keys[0], cached_prefix_values[0]
    )
    part_near = later_part(
        second_kernel, tokens, 2 * slots, [],
        meta, q_near, keys, values, k_other, v_other,
    )
    back_near = passed_along(part_near, BLK, -2)
    part_far = later_part(
        third_kernel, tokens, slots, [pltpu.VMEM(q_own.shape, BF16)],
        meta, q_own, q_far, k_other, v_other,
    )
    back_far = lax.ppermute(part_far, BLK, [(i, (i - 4) % shard_count) for i in odd])
    halves = combine([part_own, back_near, part_far, back_far], z_count, tokens, heads)
    own = lax.all_to_all(halves, ("y", "Z"), split_axis=0, concat_axis=0, tiled=True)
    other = passed_along(own, "K", 1)
    partial = project(own, other, weights)
    partial = partial.reshape(-1, *partial.shape[2:])
    received = lax.all_to_all(partial, HEADS, split_axis=0, concat_axis=0, tiled=True)
    summed = totals(received, z_count // 2)
    pairs = []
    for y in range(2):
        for x in range(lax.axis_size("x")):
            for big in range(y_count):
                head = (big // 2) * 4 + (big % 2) * 2 + x % 2
                target = head * y_count + y * 2 + x // 2
                pairs.append(((y * 4 + x) * y_count + big, target))
    return lax.ppermute(summed, ("y", "x", "Y"), pairs)


def solution(mesh):
    finer = Mesh(mesh.devices.reshape(2, 4, 4, 8, 2), HEADS + BLK)
    placed = (
        P(BLK, HEADS, None),
        P(HEADS, BLK, None),
        P(HEADS, BLK, None),
        P(),
        P(),
        P(HEADS, BLK),
    )

    return jax.shard_map(
        on_device, mesh=finer, in_specs=placed, out_specs=P(HEADS, BLK), check_vma=False
    )
```
